32 devices in a mesh: dp: 8 (over z, x), view: 2 (over core), mp: 2 (over y).
Axes of the slice: x: 2, y: 2, z: 4, core: 2. Of those that a mesh axis runs over, the one named last changes fastest.
Arguments:
- tokens: bfloat16 [8, 2, 1024, 768], P('dp', 'view', 'mp'), may hold values from -6 to 6
- partner: int32 [8], replicated, may hold values from 0 to 7, each once
- mix_weight: float32 [8], P('dp'), may hold values from 0.2 to 0.8
- video_ids: int32 [8], replicated, may hold values from 0 to 3, never falling along the last dimension, each value on 1 to 4 neighbouring positions
- view_counts: int32 [2], replicated, may hold values from 256 to 1024, as said below
- self_project: bfloat16 [2, 3, 768, 768], P('view', None, None, 'mp'), may hold values from -0.21875 to 0.21875
- self_merge: bfloat16 [2, 768, 768], P('view', 'mp'), may hold values from -4 to 4
- cross_project: bfloat16 [2, 3, 768, 768], P('view', None, None, 'mp'), may hold values from -0.21875 to 0.21875
- cross_merge: bfloat16 [2, 768, 768], P('view', 'mp'), may hold values from -4 to 4
- hidden_up: bfloat16 [2, 768, 3072], P('view', None, 'mp'), may hold values from -0.21875 to 0.21875
- hidden_down: bfloat16 [2, 3072, 768], P('view', 'mp'), may hold values from -0.109375 to 0.109375
- norm_self: float32 [2, 768], P('view'), may hold values from 0.5 to 1.5
- norm_cross: float32 [2, 768], P('view'), may hold values from 0.5 to 1.5
- norm_hidden: float32 [2, 768], P('view'), may hold values from 0.5 to 1.5
- summary_project: bfloat16 [3, 768, 768], P(None, None, 'mp'), may hold values from -0.21875 to 0.21875
- summary_merge: bfloat16 [768, 768], P('mp'), may hold values from -0.375 to 0.375
- summary_up: bfloat16 [768, 3072], P(None, 'mp'), may hold values from -0.21875 to 0.21875
- summary_down: bfloat16 [3072, 768], P('mp'), may hold values from -0.109375 to 0.109375
- summary_norm_self: float32 [768], replicated, may hold values from 0.5 to 1.5
- summary_norm_hidden: float32 [768], replicated, may hold values from 0.5 to 1.5
- tokens_cotangent: bfloat16 [8, 2, 1024, 768], P('dp', 'view', 'mp'), may hold values from -6 to 6
- summary_cotangent: float32 [8, 2, 768], replicated, may hold values from -6 to 6
Outputs:
- tokens_out: bfloat16 [8, 2, 1024, 768], P('dp', 'view', 'mp')
- summary_out: float32 [8, 2, 768], replicated
- tokens_grad: float32 [8, 2, 1024, 768], P('dp', 'view', 'mp')
- self_project_grad: float32 [2, 3, 768, 768], P('view', None, None, 'mp')
- self_merge_grad: float32 [2, 768, 768], P('view', 'mp')
- cross_project_grad: float32 [2, 3, 768, 768], P('view', None, None, 'mp')
- cross_merge_grad: float32 [2, 768, 768], P('view', 'mp')
- hidden_up_grad: float32 [2, 768, 3072], P('view', None, 'mp')
- hidden_down_grad: float32 [2, 3072, 768], P('view', 'mp')
- norm_self_grad: float32 [2, 768], P('view')
- norm_cross_grad: float32 [2, 768], P('view')
- norm_hidden_grad: float32 [2, 768], P('view')
- summary_project_grad: float32 [3, 768, 768], P(None, None, 'mp')
- summary_merge_grad: float32 [768, 768], P('mp')
- summary_up_grad: float32 [768, 3072], P(None, 'mp')
- summary_down_grad: float32 [3072, 768], P('mp')
- summary_norm_self_grad: float32 [768], replicated
- summary_norm_hidden_grad: float32 [768], replicated
The draws below stay inside these ranges and needn't reach their ends.
Inputs may be any that keep to these rules, and one draw needn't show every extreme that they name: Every clip is the partner of exactly one clip. `video_ids`: ids never fall from one clip to the next. `view_counts`: positions from a view's count on are padding; some view has all 1024 positions real.
All inputs are finite; a program needn't handle non-finite values.
Results may differ from the reference program's by a relative error of at most 0.035.
Values may be sent and summed in bfloat16 or wider, within the bound.
A program may use at most 256 MiB of HBM per device.

```python
import math
from functools import partial
import jax
import jax.numpy as jnp
import numpy as np
from jax import lax

D = 768
HEAD = 64
FF = 3072
SEQ = 1024
VIEWS = 2
CLIPS = 8


def draw_view_counts(key, part):
    counts = jax.random.randint(jax.random.fold_in(key, 11), (VIEWS,), SEQ // 4, SEQ + 1)
    longest = jax.random.randint(jax.random.fold_in(key, 12), (), 0, VIEWS)
    return jnp.where(jnp.arange(VIEWS) == longest, SEQ, counts).astype(jnp.int32)


def levels(rng, extent, shards, low, high):
    level = 1.0
    for dim, blocks in shards:
        heights = jax.random.uniform(jax.random.fold_in(jax.random.fold_in(rng, 6), dim), (blocks,), jnp.float32, low / len(shards), high / len(shards))
        level = level * jnp.repeat(jnp.exp(heights), extent[dim] // blocks).reshape((-1,) + (1,) * (len(extent) - 1 - dim))
    return level


def profile(number_of, total, most, skew):
    weights = [(1 << 20) // math.isqrt(grade ** skew) + 1 for grade in range(2, number_of + 1)]
    rest, given = total - most - (number_of - 1), [1] * (number_of - 1)
    while rest > 0:
        candidates = [i for i in range(number_of - 1) if given[i] < most]
        whole, left = sum([weights[i] for i in candidates]), rest
        for i in candidates:
            more = min(most - given[i], max(1, left * weights[i] // whole), rest)
            given[i] = given[i] + more
            rest = rest - more
    return np.array([most] + given)


def ragged_sizes(key, number_of, total, limit, slope):
    if number_of == 2:
        one = jax.random.randint(key, (), max(1, total - limit), min(limit, total - 1) + 1)
        return jnp.stack([one, total - one])
    sizes = jnp.asarray(profile(number_of, total, limit, slope), jnp.int32)
    couples = (number_of - 1) // 2
    donor, sink = sizes[1:1 + 2 * couples:2], sizes[2:2 + 2 * couples:2]
    margin = jnp.minimum(donor - 1, limit - sink)
    passed = jax.random.randint(jax.random.fold_in(key, 1), (couples,), 0, 1 << 20) % (margin + 1)
    sizes = sizes.at[1:1 + 2 * couples:2].set(donor - passed).at[2:2 + 2 * couples:2].set(sink + passed)
    return sizes[jax.random.permutation(jax.random.fold_in(key, 2), number_of)]


def bell_draw(own_key, extent, scale, reach, split=(), kind=jnp.bfloat16):
    drawn = jax.random.normal(own_key, extent, jnp.float32) * scale
    if len(split) > 0:
        drawn = levels(own_key, extent, split, -0.22, 0.18) * drawn
    return jnp.clip(drawn, min=-reach, max=reach).astype(kind)


def setup_inputs(seed: int = 0) -> dict:
    seeds = jax.random.split(jax.random.key(seed), 23)
    tokens = bell_draw(seeds[0], (CLIPS, VIEWS, SEQ, D), 1.0, 6.0, ((0, 8), (1, 2), (2, 2)))
    partner = jax.random.permutation(seeds[1], CLIPS).astype(jnp.int32)
    mix_weight = jnp.clip(0.2 + 0.6 * jax.random.uniform(seeds[2], (CLIPS,), jnp.float32) ** levels(seeds[2], (CLIPS,), ((0, 8),), -0.2, 0.2), 0.2, 0.8)
    video_ids = jnp.searchsorted(jnp.cumsum(ragged_sizes(seeds[3], max(1, CLIPS // 2), CLIPS, min(4, max(2, CLIPS // 2)), 0)), jnp.arange(CLIPS), side="right").astype(jnp.int32)
    view_counts = draw_view_counts(jax.random.fold_in(seeds[22], 71), 0)
    self_project = bell_draw(seeds[5], (VIEWS, 3, D, D), D ** -0.5, 0.21875, ((0, 2), (3, 2)))
    self_merge = bell_draw(seeds[6], (VIEWS, D, D), (3 * D // SEQ) ** -0.5, 4.0, ((0, 2), (1, 2)))
    cross_project = bell_draw(seeds[7], (VIEWS, 3, D, D), D ** -0.5, 0.21875, ((0, 2), (3, 2)))
    cross_merge = bell_draw(seeds[8], (VIEWS, D, D), (3 * D // SEQ) ** -0.5, 4.0, ((0, 2), (1, 2)))
    hidden_up = bell_draw(seeds[9], (VIEWS, D, FF), D ** -0.5, 0.21875, ((0, 2), (2, 2)))
    hidden_down = bell_draw(seeds[10], (VIEWS, FF, D), FF ** -0.5, 0.109375, ((0, 2), (1, 2)))
    norm_self = jnp.clip(1.0 + 0.1 * jax.random.normal(seeds[11], (VIEWS, D), jnp.float32), 0.5, 1.5)
    norm_cross = jnp.clip(1.0 + 0.1 * jax.random.normal(seeds[12], (VIEWS, D), jnp.float32), 0.5, 1.5)
    norm_hidden = jnp.clip(1.0 + 0.1 * jax.random.normal(seeds[13], (VIEWS, D), jnp.float32), 0.5, 1.5)
    summary_project = bell_draw(seeds[14], (3, D, D), D ** -0.5, 0.21875, ((2, 2),))
    summary_merge = bell_draw(seeds[15], (D, D), (D // 3) ** -0.5, 0.375, ((0, 2),))
    summary_up = bell_draw(seeds[16], (D, FF), D ** -0.5, 0.21875, ((1, 2),))
    summary_down = bell_draw(seeds[17], (FF, D), FF ** -0.5, 0.109375, ((0, 2),))
    summary_norm_self = jnp.clip(1.0 + 0.1 * jax.random.normal(seeds[18], (D,), jnp.float32), 0.5, 1.5)
    summary_norm_hidden = jnp.clip(1.0 + 0.1 * jax.random.normal(seeds[19], (D,), jnp.float32), 0.5, 1.5)
    tokens_cotangent = bell_draw(seeds[20], (CLIPS, VIEWS, SEQ, D), 1.0, 6.0, ((0, 8), (1, 2), (2, 2)))
    summary_cotangent = bell_draw(seeds[21], (CLIPS, VIEWS, D), 1.0, 6.0, (), jnp.float32)
    return {"tokens": tokens, "partner": partner, "mix_weight": mix_weight, "video_ids": video_ids, "view_counts": view_counts, "self_project": self_project, "self_merge": self_merge, "cross_project": cross_project, "cross_merge": cross_merge, "hidden_up": hidden_up, "hidden_down": hidden_down, "norm_self": norm_self, "norm_cross": norm_cross, "norm_hidden": norm_hidden, "summary_project": summary_project, "summary_merge": summary_merge, "summary_up": summary_up, "summary_down": summary_down, "summary_norm_self": summary_norm_self, "summary_norm_hidden": summary_norm_hidden, "tokens_cotangent": tokens_cotangent, "summary_cotangent": summary_cotangent}


EPS = 1e-05
NEG = -1000000000.0
HIGH = lax.Precision.HIGHEST

@jax.custom_vjp
def low(v):
    return lax.optimization_barrier(v.astype(jnp.bfloat16)).astype(jnp.float32)

@jax.custom_vjp
def low_back(v):
    return v

def low_keep(v):
    return (low(v), None)

def low_pass(kept, grad):
    return (grad,)

def back_keep(v):
    return (v, None)

def back_low(kept, grad):
    return (low(grad),)
low.defvjp(low_keep, low_pass)
low_back.defvjp(back_keep, back_low)

def layer_norm(rows, gain):
    center = rows - lax.optimization_barrier(jnp.mean(rows, -1, keepdims=True))
    spread = lax.optimization_barrier(jnp.mean(center * center, -1, keepdims=True))
    return center * lax.rsqrt(spread + EPS) * gain

def project(rows, weight):
    return jnp.einsum('...d,de->...e', rows, weight, precision=HIGH)

def split_heads(rows):
    return rows.reshape(rows.shape[:-1] + (rows.shape[-1] // HEAD, HEAD))

def attention(query, key_rows, value_rows, valid):
    scores = low_back(jnp.einsum('qhe,khe->hqk', split_heads(query), split_heads(key_rows), precision=HIGH))
    scores = jnp.where(valid, scores, NEG)
    highest = lax.optimization_barrier(jnp.max(scores, -1, keepdims=True))
    raised = jnp.exp(scores - highest)
    probability = low(raised / lax.optimization_barrier(jnp.sum(raised, -1, keepdims=True)))
    joined = jnp.einsum('hqk,khe->qhe', probability, split_heads(value_rows), precision=HIGH)
    return low(low_back(joined.reshape(query.shape)))

def attend_rows(query_source, key_source, project_weight, valid):
    scale = HEAD ** (-0.5)
    query = low(low_back(project(query_source, project_weight[0]) * scale))
    key_rows = low(low_back(project(key_source, project_weight[1])))
    value_rows = low(low_back(project(key_source, project_weight[2])))
    return attention(query, key_rows, value_rows, valid)

def self_branch(rows, project_weight, merge_weight, gain, valid):
    normed = low(layer_norm(rows, gain))
    return rows + low_back(project(attend_rows(normed, normed, project_weight, valid), merge_weight))

def cross_branch(inputs, project_weight, merge_weight, valid):
    rows, own_normed, next_normed = inputs
    return rows + low_back(project(attend_rows(own_normed, next_normed, project_weight, valid), merge_weight))

def gelu_exact(values):
    return jax.nn.gelu(values, approximate=False)

def hidden_branch(rows, up_weight, down_weight, gain):
    normed = low(layer_norm(rows, gain))
    hidden = low(gelu_exact(low_back(project(normed, up_weight))))
    return rows + low_back(project(hidden, down_weight))

def reference(tokens, partner, mix_weight, video_ids, view_counts, self_project, self_merge, cross_project, cross_merge, hidden_up, hidden_down, norm_self, norm_cross, norm_hidden, summary_project, summary_merge, summary_up, summary_down, summary_norm_self, summary_norm_hidden, tokens_cotangent, summary_cotangent):
    positions = jnp.arange(SEQ)
    token_video = jnp.repeat(video_ids, VIEWS)
    summary_valid = (token_video[:, None] == token_video[None, :])[None]

    def forward(token_values, project_self, merge_self, project_cross, merge_cross, up_values, down_values, gain_self, gain_cross, gain_hidden, project_top, merge_top, up_top, down_top, gain_top, gain_last):
        mixing = mix_weight[:, None, None, None]
        mixed = mixing * token_values + (1.0 - mixing) * low_back(token_values[partner])
        firsts = []
        for view in range(VIEWS):
            valid = (positions < view_counts[view])[None, None, :]
            branch = partial(self_branch, project_weight=project_self[view], merge_weight=merge_self[view], gain=gain_self[view], valid=valid)
            firsts.append(lax.map(jax.checkpoint(branch), mixed[:, view]))
        first = jnp.stack(firsts, 1)
        normed_cross = low(layer_norm(first, gain_cross[None, :, None, :]))
        rolled = jnp.roll(normed_cross, -1, axis=1)
        seconds = []
        for view in range(VIEWS):
            valid = (positions < view_counts[(view + 1) % VIEWS])[None, None, :]
            branch = partial(cross_branch, project_weight=project_cross[view], merge_weight=merge_cross[view], valid=valid)
            seconds.append(lax.map(jax.checkpoint(branch), (first[:, view], normed_cross[:, view], rolled[:, view])))
        second = jnp.stack(seconds, 1)
        thirds = []
        for view in range(VIEWS):
            branch = partial(hidden_branch, up_weight=up_values[view], down_weight=down_values[view], gain=gain_hidden[view])
            thirds.append(lax.map(jax.checkpoint(branch), second[:, view]))
        third = jnp.stack(thirds, 1)
        class_rows = third[:, :, 0, :].reshape(CLIPS * VIEWS, D)
        summary_mid = self_branch(class_rows, project_top, merge_top, gain_top, summary_valid)
        summary = hidden_branch(summary_mid, up_top, down_top, gain_last)
        return (third, summary.reshape(CLIPS, VIEWS, D))
    floats = tuple((values.astype(jnp.float32) for values in (tokens, self_project, self_merge, cross_project, cross_merge, hidden_up, hidden_down, norm_self, norm_cross, norm_hidden, summary_project, summary_merge, summary_up, summary_down, summary_norm_self, summary_norm_hidden)))
    outputs, pullback = jax.vjp(forward, *floats)
    grads = pullback((tokens_cotangent.astype(jnp.float32), summary_cotangent.astype(jnp.float32)))
    return (outputs[0].astype(jnp.bfloat16), outputs[1], grads[0], grads[1], grads[2], grads[3], grads[4], grads[5], grads[6], grads[7], grads[8], grads[9], grads[10], grads[11], grads[12], grads[13], grads[14], grads[15])
```

```python
import functools

import jax
import jax.numpy as jnp
from jax import lax
from jax.experimental import pallas as pl
from jax.experimental.pallas import tpu as pltpu
from jax.sharding import PartitionSpec as P

D = 768
HEAD = 64
MESH = pl.DeviceIdType.MESH


EPS = 1e-05
NEG = -1000000000.0


def shifted(value, axis, steps):
    count = lax.axis_size(axis)
    pairs = [(source, (source + steps) % count) for source in range(count)]
    return lax.ppermute(value, axis, pairs)


def layer_norm(rows, gain):
    center = rows - jnp.mean(rows, -1, keepdims=True)
    inverse = lax.rsqrt(jnp.mean(center * center, -1, keepdims=True) + EPS)
    unit = center * inverse
    return (unit * gain, unit, inverse)


def layer_norm_back(grad_out, unit, inverse, gain):
    gain_grad = jnp.sum(grad_out * unit, axis=tuple(range(grad_out.ndim - 1)))
    scaled = grad_out * gain
    centered = scaled - jnp.mean(scaled, -1, keepdims=True)
    return (inverse * (centered - unit * jnp.mean(scaled * unit, -1, keepdims=True)), gain_grad)


def gelu_exact(values):
    return jax.nn.gelu(values, approximate=False)


def product(left, right, form):
    return jnp.einsum(form, left, right, preferred_element_type=jnp.float32)


def split_heads(rows):
    return rows.reshape(rows.shape[:-1] + (rows.shape[-1] // HEAD, HEAD))


def merge_heads(rows):
    return rows.reshape(rows.shape[:-2] + (rows.shape[-2] * rows.shape[-1],))


def peer_of(axes, index):
    place = {}
    for axis in reversed(axes):
        count = lax.axis_size(axis)
        place[axis] = index % count
        index = index // count
    return place


def flat_index(axes):
    index = 0
    for axis in axes:
        index = index * lax.axis_size(axis) + lax.axis_index(axis)
    return index


def trade_kernel(axes, total, split, source, target, send_sem, recv_sem, own_sem):
    me = flat_index(axes)
    barrier = pltpu.get_barrier_semaphore()
    for step in range(1, total):
        peer = peer_of(axes, (me + step) % total)
        pl.semaphore_signal(barrier, inc=1, device_id=peer, device_id_type=MESH)
    pl.semaphore_wait(barrier, total - 1)

    def piece(index):
        return source.at[index] if split else source

    own = pltpu.make_async_copy(piece(me), target.at[me], own_sem)
    own.start()
    copies = []
    for step in range(1, total):
        to = (me + step) % total
        copies.append(
            pltpu.make_async_remote_copy(
                src_ref=piece(to),
                dst_ref=target.at[me],
                send_sem=send_sem.at[step],
                recv_sem=recv_sem.at[step],
                device_id=peer_of(axes, to),
                device_id_type=MESH,
            )
        )
        copies[-1].start()
    own.wait()
    for copy in copies:
        copy.wait()


def trade(value, axes, split, collective_id):
    total = 1
    for axis in axes:
        total *= lax.axis_size(axis)
    piece = value.shape[1:] if split else value.shape
    return pl.pallas_call(
        functools.partial(trade_kernel, axes, total, split),
        out_shape=jax.ShapeDtypeStruct((total,) + piece, value.dtype),
        in_specs=[pl.BlockSpec(memory_space=pltpu.VMEM)],
        out_specs=pl.BlockSpec(memory_space=pltpu.VMEM),
        scratch_shapes=[
            pltpu.SemaphoreType.DMA((total,)),
            pltpu.SemaphoreType.DMA((total,)),
            pltpu.SemaphoreType.DMA,
        ],
        compiler_params=pltpu.CompilerParams(collective_id=collective_id, has_side_effects=True),
    )(value)


def clip_rows(rows, wanted, collective_id):
    count = lax.axis_size("dp")
    clips, length, width = rows.shape
    pieces = jnp.swapaxes(rows.reshape(clips, count, length // count, width), 0, 1)
    held = trade(pieces, ("dp",), True, collective_id)
    held = held.reshape(count * clips, length // count, width)
    picked = jnp.concatenate(
        [lax.dynamic_slice_in_dim(held, wanted[clip], 1) for clip in range(count * clips)]
    )
    back = trade(picked.reshape(pieces.shape), ("dp",), True, collective_id + 1)
    return jnp.swapaxes(back, 0, 1).reshape(rows.shape)


def row_blocks(piece):
    count = lax.axis_size("mp")
    return [piece] + [shifted(piece, "mp", -step) for step in range(1, count)]


def own_sum(parts):
    total = parts[0]
    for step in range(1, len(parts)):
        total = total + shifted(parts[step].astype(jnp.bfloat16), "mp", step).astype(jnp.float32)
    return total


def whole_sum(value):
    parts = jnp.stack(row_blocks(value))
    if parts.shape[0] > 2:
        parts = jnp.roll(parts, lax.axis_index("mp"), 0)
    return jnp.sum(parts, 0)


def far_first(count):
    return list(range(1, count)) + [0]


def attend_block(query_block, key_rows, value_rows, valid):
    scores = jnp.where(valid, product(query_block, key_rows, "cqhe,ckhe->chqk"), NEG)
    highest = jnp.max(scores, -1, keepdims=True)
    raised = jnp.exp(scores - highest)
    totals = jnp.sum(raised, -1, keepdims=True)
    weights = (raised / totals).astype(jnp.bfloat16)
    result = product(weights, value_rows, "chqk,ckhe->cqhe").astype(jnp.bfloat16)
    return (result, highest + jnp.log(totals))


def attend_block_back(query_block, key_rows, value_rows, valid, grad_block, log_sums):
    scores = jnp.where(valid, product(query_block, key_rows, "cqhe,ckhe->chqk"), NEG)
    weights = jnp.exp(scores - log_sums)
    grad_weights = product(grad_block, value_rows, "cqhe,ckhe->chqk")
    grad_scores = (
        weights * (grad_weights - jnp.sum(weights * grad_weights, -1, keepdims=True))
    ).astype(jnp.bfloat16)
    query_grad = product(grad_scores, key_rows, "chqk,ckhe->cqhe").astype(jnp.bfloat16)
    key_grad = product(grad_scores, query_block, "chqk,cqhe->ckhe")
    value_grad = product(weights.astype(jnp.bfloat16), grad_block, "chqk,cqhe->ckhe")
    return (query_grad, key_grad, value_grad)


def attend(queries, keys, values, valid):
    key_rows = split_heads(jnp.concatenate(keys, 1))
    value_rows = split_heads(jnp.concatenate(values, 1))
    heads = [None] * len(queries)
    sums = [None] * len(queries)
    for j in far_first(len(queries)):
        result, sums[j] = attend_block(split_heads(queries[j]), key_rows, value_rows, valid)
        heads[j] = merge_heads(result)
    return (heads, sums)


def attend_back(queries, keys, values, valid, grads, sums):
    key_rows = split_heads(jnp.concatenate(keys, 1))
    value_rows = split_heads(jnp.concatenate(values, 1))
    query_grads = [None] * len(queries)
    key_grad = value_grad = 0.0
    for j in far_first(len(queries)):
        query_grad, key_term, value_term = attend_block_back(
            split_heads(queries[j]), key_rows, value_rows, valid, split_heads(grads[j]), sums[j]
        )
        query_grads[j] = merge_heads(query_grad)
        key_grad = key_grad + key_term
        value_grad = value_grad + value_term
    parts = len(keys)
    return (
        query_grads,
        jnp.split(merge_heads(key_grad.astype(jnp.bfloat16)), parts, 1),
        jnp.split(merge_heads(value_grad.astype(jnp.bfloat16)), parts, 1),
    )


def project_rows(source, weight):
    return product(source, weight, "csd,de->cse")


def query_rows(source, weight):
    return (project_rows(source, weight) * HEAD ** (-0.5)).astype(jnp.bfloat16)


def back_rows(grad, weight):
    return product(grad, weight, "cse,de->csd")


def weight_sums(sources, grads):
    return sum(product(source, grad, "csd,cse->de") for source, grad in zip(sources, grads))


def scaled_grads(grads):
    return [grad * HEAD ** (-0.5) for grad in grads]


def summary_layer(
    summary_rows, top_grad, weights, gain_top, gain_last, summary_valid
):
    use_project, use_merge, use_up, use_down = weights
    top_normed, top_unit, top_inverse = layer_norm(summary_rows, gain_top)
    top_low = top_normed.astype(jnp.bfloat16)[None]
    top_query = query_rows(top_low, use_project[0])
    top_key = project_rows(top_low, use_project[1]).astype(jnp.bfloat16)
    top_value = project_rows(top_low, use_project[2]).astype(jnp.bfloat16)
    (top_flat,), top_sums = attend([top_query], [top_key], [top_value], summary_valid)
    summary_mid = summary_rows + whole_sum(product(top_flat, use_merge, "cse,ed->csd")[0])
    mid_normed, mid_unit, mid_inverse = layer_norm(summary_mid, gain_last)
    mid_low = mid_normed.astype(jnp.bfloat16)[None]
    top_before = product(mid_low, use_up, "csd,df->csf")
    top_hidden = gelu_exact(top_before).astype(jnp.bfloat16)
    summary_final = summary_mid + whole_sum(product(top_hidden, use_down, "csf,fd->csd")[0])
    down_input = top_grad.astype(jnp.bfloat16)[None]
    down_grad = product(top_hidden, down_input, "csf,csd->fd")
    act_grad = jax.vjp(gelu_exact, top_before)[1](product(down_input, use_down, "csd,fd->csf"))[
        0
    ].astype(jnp.bfloat16)
    up_grad = product(mid_low, act_grad, "csd,csf->df")
    mid_rows_grad, last_gain_grad = layer_norm_back(
        whole_sum(product(act_grad, use_up, "csf,df->csd")[0]), mid_unit, mid_inverse, gain_last
    )
    mid_grad = top_grad + mid_rows_grad
    merge_input = mid_grad.astype(jnp.bfloat16)[None]
    merge_grad = product(top_flat, merge_input, "cse,csd->ed")
    top_heads_grad = product(merge_input, use_merge, "csd,ed->cse").astype(jnp.bfloat16)
    (query_grad,), (key_grad,), (value_grad,) = attend_back(
        [top_query], [top_key], [top_value], summary_valid, [top_heads_grad], top_sums
    )
    query_grad = query_grad * HEAD ** (-0.5)
    project_grad = jnp.stack(
        [product(top_low, grad, "csd,cse->de") for grad in (query_grad, key_grad, value_grad)]
    )
    project_terms = (
        back_rows(query_grad, use_project[0])
        + back_rows(key_grad, use_project[1])
        + back_rows(value_grad, use_project[2])
    )
    first_top_grad, top_gain_grad = layer_norm_back(
        whole_sum(project_terms[0]), top_unit, top_inverse, gain_top
    )
    class_grad = mid_grad + first_top_grad
    return (
        summary_final,
        class_grad,
        (project_grad, merge_grad, up_grad, down_grad),
        top_gain_grad,
        last_gain_grad,
    )


def shards(
    tokens,
    partner,
    mix_weight,
    video_ids,
    view_counts,
    self_project,
    self_merge,
    cross_project,
    cross_merge,
    hidden_up,
    hidden_down,
    norm_self,
    norm_cross,
    norm_hidden,
    summary_project,
    summary_merge,
    summary_up,
    summary_down,
    summary_norm_self,
    summary_norm_hidden,
    tokens_cotangent,
    summary_cotangent,
):
    local_tokens = tokens[:, 0]
    clip_count = local_tokens.shape[0]
    data_index = lax.axis_index("dp")
    view_index = lax.axis_index("view")
    model_index = lax.axis_index("mp")
    view_total = lax.axis_size("view")
    model_total = lax.axis_size("mp")
    clip_total = clip_count * lax.axis_size("dp")
    length = local_tokens.shape[1]
    order = far_first(model_total)
    own_clips = data_index * clip_count + jnp.arange(clip_count, dtype=jnp.int32)
    partner_tokens = clip_rows(local_tokens, partner, 0).astype(jnp.float32)
    grad_blocks = row_blocks(tokens_cotangent[:, 0])
    mixing = mix_weight[:, None, None]
    mixed_rows = mixing * local_tokens.astype(jnp.float32) + (1.0 - mixing) * partner_tokens
    owners = [(model_index + step) % model_total for step in range(model_total)]
    positions = jnp.concatenate([owner * length + jnp.arange(length) for owner in owners])
    own_valid = (positions < view_counts[view_index])[None, None, None, :]
    next_valid = (positions < view_counts[(view_index + 1) % view_total])[None, None, None, :]

    normed_self, unit_self, inverse_self = layer_norm(mixed_rows, norm_self[0])
    self_blocks = row_blocks(normed_self.astype(jnp.bfloat16))
    self_weights = self_project[0]
    self_queries = [query_rows(block, self_weights[0]) for block in self_blocks]
    self_keys = [project_rows(block, self_weights[1]).astype(jnp.bfloat16) for block in self_blocks]
    self_values = [
        project_rows(block, self_weights[2]).astype(jnp.bfloat16) for block in self_blocks
    ]
    self_heads, self_sums = attend(self_queries, self_keys, self_values, own_valid)
    first_rows = mixed_rows + own_sum(
        [product(heads, self_merge[0], "cse,ed->csd") for heads in self_heads]
    )

    normed_cross, unit_cross, inverse_cross = layer_norm(first_rows, norm_cross[0])
    cross_blocks = row_blocks(normed_cross.astype(jnp.bfloat16))
    next_blocks = [shifted(block, "view", -1) for block in cross_blocks]
    cross_weights = cross_project[0]
    cross_queries = [query_rows(block, cross_weights[0]) for block in cross_blocks]
    cross_keys = [
        project_rows(block, cross_weights[1]).astype(jnp.bfloat16) for block in next_blocks
    ]
    cross_values = [
        project_rows(block, cross_weights[2]).astype(jnp.bfloat16) for block in next_blocks
    ]
    cross_heads, cross_sums = attend(cross_queries, cross_keys, cross_values, next_valid)
    second_rows = first_rows + own_sum(
        [product(heads, cross_merge[0], "cse,ed->csd") for heads in cross_heads]
    )

    normed_hidden, unit_hidden, inverse_hidden = layer_norm(second_rows, norm_hidden[0])
    hidden_blocks = row_blocks(normed_hidden.astype(jnp.bfloat16))
    befores = [product(block, hidden_up[0], "csd,df->csf") for block in hidden_blocks]
    hiddens = [gelu_exact(before).astype(jnp.bfloat16) for before in befores]
    third_rows = second_rows + own_sum(
        [product(hidden, hidden_down[0], "csf,fd->csd") for hidden in hiddens]
    )

    everyone = ("dp", "view", "mp")
    class_all = trade(third_rows[:, 0, :], everyone, False, 2)
    class_all = class_all.reshape(clip_total // clip_count, view_total, model_total, clip_count, D)
    class_grid = jnp.swapaxes(class_all[:, :, 0], 1, 2).reshape(clip_total, view_total, D)
    row_total = clip_total * view_total
    token_video = jnp.repeat(video_ids, view_total)
    summary_valid = (token_video[:, None] == token_video[None, :])[None, None]
    summary_final, class_flat, summary_grads, summary_norm_self_grad, summary_norm_hidden_grad = (
        summary_layer(
            class_grid.reshape(row_total, D),
            summary_cotangent.reshape(row_total, D),
            (summary_project, summary_merge, summary_up, summary_down),
            summary_norm_self,
            summary_norm_hidden,
            summary_valid,
        )
    )
    summary_project_grad, summary_merge_grad, summary_up_grad, summary_down_grad = summary_grads
    summary_out = summary_final.reshape(clip_total, view_total, D)
    clip_match = (jnp.arange(clip_total, dtype=jnp.int32)[:, None] == own_clips[None, :]).astype(
        jnp.float32
    )
    view_match = (jnp.arange(view_total) == view_index).astype(jnp.float32)
    class_grad = class_flat.reshape(clip_total, view_total, D)
    view_pick = jnp.sum(class_grad * view_match[None, :, None], axis=1)
    own_class = jnp.sum(clip_match[:, :, None] * view_pick[:, None, :], axis=0)

    third_grads = [
        block.astype(jnp.float32).at[:, 0].add(own_class * (owner == 0).astype(jnp.float32))
        for block, owner in zip(grad_blocks, owners)
    ]
    third_grad = third_grads[0]
    down_rows = [block.astype(jnp.bfloat16) for block in third_grads]
    act_grads = [
        jax.vjp(gelu_exact, before)[1](product(rows, hidden_down[0], "csd,fd->csf"))[0].astype(
            jnp.bfloat16
        )
        for before, rows in zip(befores, down_rows)
    ]
    hidden_norm_grad = own_sum(
        [product(act_grad, hidden_up[0], "csf,df->csd") for act_grad in act_grads]
    )
    down_grad = sum(product(h, r, "csf,csd->fd") for h, r in zip(hiddens, down_rows))
    up_grad = sum(product(b, g, "csd,csf->df") for b, g in zip(hidden_blocks, act_grads))
    up_sum, down_sum = lax.psum(
        (up_grad.astype(jnp.bfloat16), down_grad.astype(jnp.bfloat16)), "dp"
    )
    rows_grad_hidden, gain_hidden_grad = layer_norm_back(
        hidden_norm_grad, unit_hidden, inverse_hidden, norm_hidden[0]
    )
    second_grad = third_grad + rows_grad_hidden

    merge_blocks = row_blocks(second_grad.astype(jnp.bfloat16))
    heads_grads = [
        product(block, cross_merge[0], "csd,ed->cse").astype(jnp.bfloat16)
        for block in merge_blocks
    ]
    query_grads, key_grads, value_grads = attend_back(
        cross_queries, cross_keys, cross_values, next_valid, heads_grads, cross_sums
    )
    query_grads = scaled_grads(query_grads)
    terms = [None] * model_total
    for step in order:
        next_term = back_rows(key_grads[step], cross_weights[1]) + back_rows(
            value_grads[step], cross_weights[2]
        )
        returned = shifted(next_term.astype(jnp.bfloat16), "view", 1).astype(jnp.float32)
        terms[step] = back_rows(query_grads[step], cross_weights[0]) + returned
    cross_norm_grad = own_sum(terms)
    cross_merge_grad = weight_sums(cross_heads, merge_blocks)
    cross_project_grad = jnp.stack(
        [
            weight_sums(cross_blocks, query_grads),
            weight_sums(next_blocks, key_grads),
            weight_sums(next_blocks, value_grads),
        ]
    )
    cross_low = (cross_project_grad.astype(jnp.bfloat16), cross_merge_grad.astype(jnp.bfloat16))
    cross_low, (up_sum, down_sum) = lax.optimization_barrier((cross_low, (up_sum, down_sum)))
    cross_project_sum, cross_merge_sum = lax.psum(cross_low, "dp")
    rows_grad_cross, gain_cross_grad = layer_norm_back(
        cross_norm_grad, unit_cross, inverse_cross, norm_cross[0]
    )
    first_grad = second_grad + rows_grad_cross

    merge_blocks = row_blocks(first_grad.astype(jnp.bfloat16))
    heads_grads = [
        product(block, self_merge[0], "csd,ed->cse").astype(jnp.bfloat16) for block in merge_blocks
    ]
    query_grads, key_grads, value_grads = attend_back(
        self_queries, self_keys, self_values, own_valid, heads_grads, self_sums
    )
    query_grads = scaled_grads(query_grads)
    self_norm_grad = own_sum(
        [
            back_rows(query_grads[step], self_weights[0])
            + back_rows(key_grads[step], self_weights[1])
            + back_rows(value_grads[step], self_weights[2])
            for step in range(model_total)
        ]
    )
    self_merge_grad = weight_sums(self_heads, merge_blocks)
    self_project_grad = jnp.stack(
        [
            weight_sums(self_blocks, query_grads),
            weight_sums(self_blocks, key_grads),
            weight_sums(self_blocks, value_grads),
        ]
    )
    self_low = (self_project_grad.astype(jnp.bfloat16), self_merge_grad.astype(jnp.bfloat16))
    self_low, (cross_project_sum, cross_merge_sum) = lax.optimization_barrier(
        (self_low, (cross_project_sum, cross_merge_sum))
    )
    self_project_sum, self_merge_sum = lax.psum(self_low, "dp")
    rows_grad_self, gain_self_grad = layer_norm_back(
        self_norm_grad, unit_self, inverse_self, norm_self[0]
    )
    mixed_grad = first_grad + rows_grad_self
    gains = jnp.stack([gain_self_grad, gain_cross_grad, gain_hidden_grad])
    gains = jnp.sum(trade(gains, ("dp", "mp"), False, 3), 0)

    sent_rows = ((1.0 - mixing) * mixed_grad).astype(jnp.bfloat16)
    clips = jnp.arange(clip_total, dtype=jnp.int32)
    inverse_partner = jnp.sum(
        jnp.where(partner[None, :] == clips[:, None], clips[None, :], 0), 1
    )
    returned_rows = clip_rows(sent_rows, inverse_partner, 4).astype(jnp.float32)
    tokens_grad = (mixing * mixed_grad + returned_rows)[:, None]
    tokens_out = third_rows.astype(jnp.bfloat16)[:, None]
    return (
        tokens_out,
        summary_out,
        tokens_grad,
        self_project_sum.astype(jnp.float32)[None],
        self_merge_sum.astype(jnp.float32)[None],
        cross_project_sum.astype(jnp.float32)[None],
        cross_merge_sum.astype(jnp.float32)[None],
        up_sum.astype(jnp.float32)[None],
        down_sum.astype(jnp.float32)[None],
        gains[0][None],
        gains[1][None],
        gains[2][None],
        summary_project_grad,
        summary_merge_grad,
        summary_up_grad,
        summary_down_grad,
        summary_norm_self_grad,
        summary_norm_hidden_grad,
    )


def solution(mesh):
    in_specs = (
        P("dp", "view", "mp", None),
        P(),
        P("dp"),
        P(),
        P(),
        P("view", None, None, "mp"),
        P("view", "mp", None),
        P("view", None, None, "mp"),
        P("view", "mp", None),
        P("view", None, "mp"),
        P("view", "mp", None),
        P("view", None),
        P("view", None),
        P("view", None),
        P(None, None, "mp"),
        P("mp", None),
        P(None, "mp"),
        P("mp", None),
        P(),
        P(),
        P("dp", "view", "mp", None),
        P(),
    )
    out_specs = (
        P("dp", "view", "mp", None),
        P(),
        P("dp", "view", "mp", None),
        P("view", None, None, "mp"),
        P("view", "mp", None),
        P("view", None, None, "mp"),
        P("view", "mp", None),
        P("view", None, "mp"),
        P("view", "mp", None),
        P("view", None),
        P("view", None),
        P("view", None),
        P(None, None, "mp"),
        P("mp", None),
        P(None, "mp"),
        P("mp", None),
        P(),
        P(),
    )
    return jax.shard_map(shards, mesh=mesh, in_specs=in_specs, out_specs=out_specs, check_vma=False)
```

```python
import functools

import jax
import jax.numpy as jnp
from jax import lax
from jax.experimental import pallas as pl
from jax.experimental.pallas import tpu as pltpu
from jax.sharding import PartitionSpec as P

D = 768
HEAD = 64
MESH = pl.DeviceIdType.MESH


EPS = 1e-05
NEG = -1000000000.0


def shifted(value, axis, steps):
    count = lax.axis_size(axis)
    pairs = [(source, (source + steps) % count) for source in range(count)]
    return lax.ppermute(value, axis, pairs)


def layer_norm(rows, gain):
    center = rows - jnp.mean(rows, -1, keepdims=True)
    inverse = lax.rsqrt(jnp.mean(center * center, -1, keepdims=True) + EPS)
    unit = center * inverse
    return (unit * gain, unit, inverse)


def layer_norm_back(grad_out, unit, inverse, gain):
    gain_grad = jnp.sum(grad_out * unit, axis=tuple(range(grad_out.ndim - 1)))
    scaled = grad_out * gain
    centered = scaled - jnp.mean(scaled, -1, keepdims=True)
    return (inverse * (centered - unit * jnp.mean(scaled * unit, -1, keepdims=True)), gain_grad)


def gelu_exact(values):
    return jax.nn.gelu(values, approximate=False)


def product(left, right, form):
    return jnp.einsum(form, left, right, preferred_element_type=jnp.float32)


def split_heads(rows):
    return rows.reshape(rows.shape[:-1] + (rows.shape[-1] // HEAD, HEAD))


def merge_heads(rows):
    return rows.reshape(rows.shape[:-2] + (rows.shape[-2] * rows.shape[-1],))


def peer_of(axes, index):
    place = {}
    for axis in reversed(axes):
        count = lax.axis_size(axis)
        place[axis] = index % count
        index = index // count
    return place


def flat_index(axes):
    index = 0
    for axis in axes:
        index = index * lax.axis_size(axis) + lax.axis_index(axis)
    return index


def trade_kernel(axes, total, split, source, target, send_sem, recv_sem, own_sem):
    me = flat_index(axes)
    barrier = pltpu.get_barrier_semaphore()
    for step in range(1, total):
        peer = peer_of(axes, (me + step) % total)
        pl.semaphore_signal(barrier, inc=1, device_id=peer, device_id_type=MESH)
    pl.semaphore_wait(barrier, total - 1)

    def piece(index):
        return source.at[index] if split else source

    own = pltpu.make_async_copy(piece(me), target.at[me], own_sem)
    own.start()
    copies = []
    for step in range(1, total):
        to = (me + step) % total
        copies.append(
            pltpu.make_async_remote_copy(
                src_ref=piece(to),
                dst_ref=target.at[me],
                send_sem=send_sem.at[step],
                recv_sem=recv_sem.at[step],
                device_id=peer_of(axes, to),
                device_id_type=MESH,
            )
        )
        copies[-1].start()
    own.wait()
    for copy in copies:
        copy.wait()


def trade(value, axes, split, collective_id):
    total = 1
    for axis in axes:
        total *= lax.axis_size(axis)
    piece = value.shape[1:] if split else value.shape
    return pl.pallas_call(
        functools.partial(trade_kernel, axes, total, split),
        out_shape=jax.ShapeDtypeStruct((total,) + piece, value.dtype),
        in_specs=[pl.BlockSpec(memory_space=pltpu.VMEM)],
        out_specs=pl.BlockSpec(memory_space=pltpu.VMEM),
        scratch_shapes=[
            pltpu.SemaphoreType.DMA((total,)),
            pltpu.SemaphoreType.DMA((total,)),
            pltpu.SemaphoreType.DMA,
        ],
        compiler_params=pltpu.CompilerParams(collective_id=collective_id, has_side_effects=True),
    )(value)


def pick_kernel(wanted_ref, held_ref, out_ref):
    out_ref[...] = held_ref[...]


def pick(held, wanted):
    block = (1,) + held.shape[1:]
    return pl.pallas_call(
        pick_kernel,
        grid_spec=pltpu.PrefetchScalarGridSpec(
            num_scalar_prefetch=1,
            grid=(held.shape[0],),
            in_specs=[pl.BlockSpec(block, lambda i, wanted_ref: (wanted_ref[i], 0, 0))],
            out_specs=pl.BlockSpec(block, lambda i, wanted_ref: (i, 0, 0)),
        ),
        out_shape=jax.ShapeDtypeStruct(held.shape, held.dtype),
    )(wanted, held)


def clip_rows(rows, wanted, collective_id):
    count = lax.axis_size("dp")
    clips, length, width = rows.shape
    pieces = jnp.swapaxes(rows.reshape(clips, count, length // count, width), 0, 1)
    held = trade(pieces, ("dp",), True, collective_id)
    held = held.reshape(count * clips, length // count, width)
    picked = pick(held, wanted)
    back = trade(picked.reshape(pieces.shape), ("dp",), True, collective_id + 1)
    return jnp.swapaxes(back, 0, 1).reshape(rows.shape)


def row_blocks(piece):
    count = lax.axis_size("mp")
    return [piece] + [shifted(piece, "mp", -step) for step in range(1, count)]


def own_sum(parts):
    total = parts[0]
    for step in range(1, len(parts)):
        total = total + shifted(parts[step].astype(jnp.bfloat16), "mp", step).astype(jnp.float32)
    return total


def whole_sum(value):
    parts = jnp.stack(row_blocks(value))
    if parts.shape[0] > 2:
        parts = jnp.roll(parts, lax.axis_index("mp"), 0)
    return jnp.sum(parts, 0)


def far_first(count):
    return list(range(1, count)) + [0]


def attend_block(query_block, key_rows, value_rows, valid):
    scores = jnp.where(valid, product(query_block, key_rows, "cqhe,ckhe->chqk"), NEG)
    highest = jnp.max(scores, -1, keepdims=True)
    raised = jnp.exp(scores - highest)
    totals = jnp.sum(raised, -1, keepdims=True)
    weights = (raised / totals).astype(jnp.bfloat16)
    result = product(weights, value_rows, "chqk,ckhe->cqhe").astype(jnp.bfloat16)
    return (result, highest + jnp.log(totals))


def attend_block_back(query_block, key_rows, value_rows, valid, grad_block, log_sums):
    scores = jnp.where(valid, product(query_block, key_rows, "cqhe,ckhe->chqk"), NEG)
    weights = jnp.exp(scores - log_sums)
    grad_weights = product(grad_block, value_rows, "cqhe,ckhe->chqk")
    grad_scores = (
        weights * (grad_weights - jnp.sum(weights * grad_weights, -1, keepdims=True))
    ).astype(jnp.bfloat16)
    query_grad = product(grad_scores, key_rows, "chqk,ckhe->cqhe").astype(jnp.bfloat16)
    key_grad = product(grad_scores, query_block, "chqk,cqhe->ckhe")
    value_grad = product(weights.astype(jnp.bfloat16), grad_block, "chqk,cqhe->ckhe")
    return (query_grad, key_grad, value_grad)


def joined(left, right, left_dim, right_dim):
    return lax.dot_general(
        left, right, (((left_dim,), (right_dim,)), ((), ())), preferred_element_type=jnp.float32
    )


def wide_bias(bias_ref, start, length, width):
    part = bias_ref[start : start + length, :]
    return jnp.concatenate([part] * (width // part.shape[1]), 1)


def attend_kernel(parts, chunk, query_ref, *refs):
    key_refs, value_refs = refs[:parts], refs[parts : 2 * parts]
    bias_ref, out_ref, sums_ref = refs[2 * parts :]
    length = key_refs[0].shape[1]
    for half in range(2):
        lanes = slice(HEAD * half, HEAD * half + HEAD)
        keys = [ref[0, :, lanes] for ref in key_refs]
        values = [ref[0, :, lanes] for ref in value_refs]
        for start in range(0, query_ref.shape[1], chunk):
            query = query_ref[0, start : start + chunk, lanes]
            scores = [
                joined(key, query, 1, 1) + wide_bias(bias_ref, j * length, length, chunk)
                for j, key in enumerate(keys)
            ]
            highest = functools.reduce(
                jnp.maximum, [jnp.max(score, 0, keepdims=True) for score in scores]
            )
            raised = [jnp.exp(score - highest) for score in scores]
            totals = sum(jnp.sum(part, 0, keepdims=True) for part in raised)
            result = sum(
                joined(value, part.astype(jnp.bfloat16), 0, 0)
                for value, part in zip(values, raised)
            )
            out_ref[0, start : start + chunk, lanes] = (result / totals).T.astype(jnp.bfloat16)
            sums_ref[0, 0, half : half + 1, start : start + chunk] = highest + jnp.log(totals)


def attend_back_kernel(parts, chunk, first, query_ref, grad_ref, heads_ref, sums_ref, *refs):
    key_refs, value_refs = refs[:parts], refs[parts : 2 * parts]
    bias_ref = refs[2 * parts]
    refs = refs[2 * parts + 1 :]
    held, outs = ((), refs) if first else (refs[: 2 * parts], refs[2 * parts :])
    query_grad_ref, grad_refs = outs[0], outs[1:]
    length = key_refs[0].shape[1]
    for half in range(2):
        lanes = slice(HEAD * half, HEAD * half + HEAD)
        keys = [ref[0, :, lanes] for ref in key_refs]
        values = [ref[0, :, lanes] for ref in value_refs]
        totals = [0.0 if first else ref[0, :, lanes] for ref in held] or [0.0] * (2 * parts)
        for start in range(0, query_ref.shape[1], chunk):
            rows = slice(start, start + chunk)
            query = query_ref[0, rows, lanes]
            grad = grad_ref[0, rows, lanes]
            shared = grad.astype(jnp.float32) * heads_ref[0, rows, lanes].astype(jnp.float32)
            delta = jnp.sum(shared.T, 0, keepdims=True)
            log_sums = sums_ref[0, 0, half : half + 1, rows]
            query_grad = 0.0
            for j in range(parts):
                scores = joined(keys[j], query, 1, 1) + wide_bias(
                    bias_ref, j * length, length, chunk
                )
                weights = jnp.exp(scores - log_sums)
                grad_scores = (weights * (joined(values[j], grad, 1, 1) - delta)).astype(
                    jnp.bfloat16
                )
                totals[j] = totals[j] + joined(grad_scores, query, 1, 0)
                totals[parts + j] = totals[parts + j] + joined(
                    weights.astype(jnp.bfloat16), grad, 1, 0
                )
                query_grad = query_grad + joined(keys[j], grad_scores, 0, 0)
            query_grad_ref[0, rows, lanes] = query_grad.T.astype(jnp.bfloat16)
        for total, ref in zip(totals, grad_refs):
            ref[0, :, lanes] = total.astype(ref.dtype)


def pair_spec(length):
    return pl.BlockSpec((1, length, 2 * HEAD), lambda clip, pair: (clip, 0, pair))


def sums_spec(length):
    return pl.BlockSpec((1, 1, 2, length), lambda clip, pair: (clip, pair, 0, 0))


def bias_spec(length):
    return pl.BlockSpec((length, 2 * HEAD), lambda clip, pair: (0, 0))


CHUNK = 256


def attend(queries, keys, values, bias):
    parts = len(keys)
    clips, length, width = queries[0].shape
    pairs = width // (2 * HEAD)
    heads = [None] * parts
    sums = [None] * parts
    for j in far_first(parts):
        heads[j], sums[j] = pl.pallas_call(
            functools.partial(attend_kernel, parts, min(CHUNK, length)),
            grid=(clips, pairs),
            out_shape=(
                jax.ShapeDtypeStruct((clips, length, width), jnp.bfloat16),
                jax.ShapeDtypeStruct((clips, pairs, 2, length), jnp.float32),
            ),
            in_specs=[pair_spec(length)] * (1 + 2 * parts) + [bias_spec(parts * length)],
            out_specs=(pair_spec(length), sums_spec(length)),
        )(queries[j], *keys, *values, bias)
    return (heads, sums)


def attend_back(queries, keys, values, bias, grads, heads, sums):
    parts = len(keys)
    clips, length, width = queries[0].shape
    pairs = width // (2 * HEAD)
    query_grads = []
    held = []
    for j in range(parts):
        kind = jnp.bfloat16 if j == parts - 1 else jnp.float32
        outs = pl.pallas_call(
            functools.partial(attend_back_kernel, parts, min(CHUNK, length), j == 0),
            grid=(clips, pairs),
            out_shape=[jax.ShapeDtypeStruct((clips, length, width), jnp.bfloat16)]
            + [jax.ShapeDtypeStruct((clips, length, width), kind)] * (2 * parts),
            in_specs=[pair_spec(length)] * 3
            + [sums_spec(length)]
            + [pair_spec(length)] * (2 * parts)
            + [bias_spec(parts * length)]
            + [pair_spec(length)] * len(held),
            out_specs=[pair_spec(length)] * (1 + 2 * parts),
        )(queries[j], grads[j], heads[j], sums[j], *keys, *values, bias, *held)
        query_grads.append(outs[0])
        held = list(outs[1:])
    return (query_grads, held[:parts], held[parts:])


def project_rows(source, weight):
    return product(source, weight, "csd,de->cse")


def query_rows(source, weight):
    return (project_rows(source, weight) * HEAD ** (-0.5)).astype(jnp.bfloat16)


def back_rows(grad, weight):
    return product(grad, weight, "cse,de->csd")


def weight_sums(sources, grads):
    return sum(product(source, grad, "csd,cse->de") for source, grad in zip(sources, grads))


def scaled_grads(grads):
    return [grad * HEAD ** (-0.5) for grad in grads]


def summary_layer(
    summary_rows, top_grad, weights, gain_top, gain_last, summary_valid
):
    use_project, use_merge, use_up, use_down = weights
    top_normed, top_unit, top_inverse = layer_norm(summary_rows, gain_top)
    top_low = top_normed.astype(jnp.bfloat16)[None]
    top_query = query_rows(top_low, use_project[0])
    top_key = project_rows(top_low, use_project[1]).astype(jnp.bfloat16)
    top_value = project_rows(top_low, use_project[2]).astype(jnp.bfloat16)
    top_key, top_value = split_heads(top_key), split_heads(top_value)
    top_heads, top_sums = attend_block(split_heads(top_query), top_key, top_value, summary_valid)
    top_flat = merge_heads(top_heads)
    summary_mid = summary_rows + whole_sum(product(top_flat, use_merge, "cse,ed->csd")[0])
    mid_normed, mid_unit, mid_inverse = layer_norm(summary_mid, gain_last)
    mid_low = mid_normed.astype(jnp.bfloat16)[None]
    top_before = product(mid_low, use_up, "csd,df->csf")
    top_hidden = gelu_exact(top_before).astype(jnp.bfloat16)
    summary_final = summary_mid + whole_sum(product(top_hidden, use_down, "csf,fd->csd")[0])
    down_input = top_grad.astype(jnp.bfloat16)[None]
    down_grad = product(top_hidden, down_input, "csf,csd->fd")
    act_grad = jax.vjp(gelu_exact, top_before)[1](product(down_input, use_down, "csd,fd->csf"))[
        0
    ].astype(jnp.bfloat16)
    up_grad = product(mid_low, act_grad, "csd,csf->df")
    mid_rows_grad, last_gain_grad = layer_norm_back(
        whole_sum(product(act_grad, use_up, "csf,df->csd")[0]), mid_unit, mid_inverse, gain_last
    )
    mid_grad = top_grad + mid_rows_grad
    merge_input = mid_grad.astype(jnp.bfloat16)[None]
    merge_grad = product(top_flat, merge_input, "cse,csd->ed")
    top_heads_grad = product(merge_input, use_merge, "csd,ed->cse").astype(jnp.bfloat16)
    query_grad, key_grad, value_grad = attend_block_back(
        split_heads(top_query),
        top_key,
        top_value,
        summary_valid,
        split_heads(top_heads_grad),
        top_sums,
    )
    query_grad = merge_heads(query_grad)
    key_grad = merge_heads(key_grad).astype(jnp.bfloat16)
    value_grad = merge_heads(value_grad).astype(jnp.bfloat16)
    query_grad = query_grad * HEAD ** (-0.5)
    project_grad = jnp.stack(
        [product(top_low, grad, "csd,cse->de") for grad in (query_grad, key_grad, value_grad)]
    )
    project_terms = (
        back_rows(query_grad, use_project[0])
        + back_rows(key_grad, use_project[1])
        + back_rows(value_grad, use_project[2])
    )
    first_top_grad, top_gain_grad = layer_norm_back(
        whole_sum(project_terms[0]), top_unit, top_inverse, gain_top
    )
    class_grad = mid_grad + first_top_grad
    return (
        summary_final,
        class_grad,
        (project_grad, merge_grad, up_grad, down_grad),
        top_gain_grad,
        last_gain_grad,
    )


def shards(
    tokens,
    partner,
    mix_weight,
    video_ids,
    view_counts,
    self_project,
    self_merge,
    cross_project,
    cross_merge,
    hidden_up,
    hidden_down,
    norm_self,
    norm_cross,
    norm_hidden,
    summary_project,
    summary_merge,
    summary_up,
    summary_down,
    summary_norm_self,
    summary_norm_hidden,
    tokens_cotangent,
    summary_cotangent,
):
    local_tokens = tokens[:, 0]
    clip_count = local_tokens.shape[0]
    data_index = lax.axis_index("dp")
    view_index = lax.axis_index("view")
    model_index = lax.axis_index("mp")
    view_total = lax.axis_size("view")
    model_total = lax.axis_size("mp")
    clip_total = clip_count * lax.axis_size("dp")
    length = local_tokens.shape[1]
    order = far_first(model_total)
    own_clips = data_index * clip_count + jnp.arange(clip_count, dtype=jnp.int32)
    partner_tokens = clip_rows(local_tokens, partner, 0).astype(jnp.float32)
    grad_blocks = row_blocks(tokens_cotangent[:, 0])
    mixing = mix_weight[:, None, None]
    mixed_rows = mixing * local_tokens.astype(jnp.float32) + (1.0 - mixing) * partner_tokens
    owners = [(model_index + step) % model_total for step in range(model_total)]
    positions = jnp.concatenate([owner * length + jnp.arange(length) for owner in owners])
    own_valid = positions < view_counts[view_index]
    next_valid = positions < view_counts[(view_index + 1) % view_total]
    own_bias, next_bias = (
        jnp.broadcast_to(jnp.where(valid, 0.0, NEG)[:, None], (positions.shape[0], 2 * HEAD))
        for valid in (own_valid, next_valid)
    )

    normed_self, unit_self, inverse_self = layer_norm(mixed_rows, norm_self[0])
    self_blocks = row_blocks(normed_self.astype(jnp.bfloat16))
    self_weights = self_project[0]
    self_queries = [query_rows(block, self_weights[0]) for block in self_blocks]
    self_keys = [project_rows(block, self_weights[1]).astype(jnp.bfloat16) for block in self_blocks]
    self_values = [
        project_rows(block, self_weights[2]).astype(jnp.bfloat16) for block in self_blocks
    ]
    self_heads, self_sums = attend(self_queries, self_keys, self_values, own_bias)
    first_rows = mixed_rows + own_sum(
        [product(heads, self_merge[0], "cse,ed->csd") for heads in self_heads]
    )

    normed_cross, unit_cross, inverse_cross = layer_norm(first_rows, norm_cross[0])
    cross_blocks = row_blocks(normed_cross.astype(jnp.bfloat16))
    next_blocks = [shifted(block, "view", -1) for block in cross_blocks]
    cross_weights = cross_project[0]
    cross_queries = [query_rows(block, cross_weights[0]) for block in cross_blocks]
    cross_keys = [
        project_rows(block, cross_weights[1]).astype(jnp.bfloat16) for block in next_blocks
    ]
    cross_values = [
        project_rows(block, cross_weights[2]).astype(jnp.bfloat16) for block in next_blocks
    ]
    cross_heads, cross_sums = attend(cross_queries, cross_keys, cross_values, next_bias)
    second_rows = first_rows + own_sum(
        [product(heads, cross_merge[0], "cse,ed->csd") for heads in cross_heads]
    )

    normed_hidden, unit_hidden, inverse_hidden = layer_norm(second_rows, norm_hidden[0])
    hidden_blocks = row_blocks(normed_hidden.astype(jnp.bfloat16))
    befores = [product(block, hidden_up[0], "csd,df->csf") for block in hidden_blocks]
    hiddens = [gelu_exact(before).astype(jnp.bfloat16) for before in befores]
    third_rows = second_rows + own_sum(
        [product(hidden, hidden_down[0], "csf,fd->csd") for hidden in hiddens]
    )

    everyone = ("dp", "view", "mp")
    class_all = trade(third_rows[:, 0, :], everyone, False, 2)
    class_all = class_all.reshape(clip_total // clip_count, view_total, model_total, clip_count, D)
    class_grid = jnp.swapaxes(class_all[:, :, 0], 1, 2).reshape(clip_total, view_total, D)
    row_total = clip_total * view_total
    token_video = jnp.repeat(video_ids, view_total)
    summary_valid = (token_video[:, None] == token_video[None, :])[None, None]
    summary_final, class_flat, summary_grads, summary_norm_self_grad, summary_norm_hidden_grad = (
        summary_layer(
            class_grid.reshape(row_total, D),
            summary_cotangent.reshape(row_total, D),
            (summary_project, summary_merge, summary_up, summary_down),
            summary_norm_self,
            summary_norm_hidden,
            summary_valid,
        )
    )
    summary_project_grad, summary_merge_grad, summary_up_grad, summary_down_grad = summary_grads
    summary_out = summary_final.reshape(clip_total, view_total, D)
    clip_match = (jnp.arange(clip_total, dtype=jnp.int32)[:, None] == own_clips[None, :]).astype(
        jnp.float32
    )
    view_match = (jnp.arange(view_total) == view_index).astype(jnp.float32)
    class_grad = class_flat.reshape(clip_total, view_total, D)
    view_pick = jnp.sum(class_grad * view_match[None, :, None], axis=1)
    own_class = jnp.sum(clip_match[:, :, None] * view_pick[:, None, :], axis=0)

    third_grads = [
        block.astype(jnp.float32).at[:, 0].add(own_class * (owner == 0).astype(jnp.float32))
        for block, owner in zip(grad_blocks, owners)
    ]
    third_grad = third_grads[0]
    down_rows = [block.astype(jnp.bfloat16) for block in third_grads]
    act_grads = [
        jax.vjp(gelu_exact, before)[1](product(rows, hidden_down[0], "csd,fd->csf"))[0].astype(
            jnp.bfloat16
        )
        for before, rows in zip(befores, down_rows)
    ]
    hidden_norm_grad = own_sum(
        [product(act_grad, hidden_up[0], "csf,df->csd") for act_grad in act_grads]
    )
    down_grad = sum(product(h, r, "csf,csd->fd") for h, r in zip(hiddens, down_rows))
    up_grad = sum(product(b, g, "csd,csf->df") for b, g in zip(hidden_blocks, act_grads))
    up_sum, down_sum = lax.psum(
        (up_grad.astype(jnp.bfloat16), down_grad.astype(jnp.bfloat16)), "dp"
    )
    rows_grad_hidden, gain_hidden_grad = layer_norm_back(
        hidden_norm_grad, unit_hidden, inverse_hidden, norm_hidden[0]
    )
    second_grad = third_grad + rows_grad_hidden

    merge_blocks = row_blocks(second_grad.astype(jnp.bfloat16))
    heads_grads = [
        product(block, cross_merge[0], "csd,ed->cse").astype(jnp.bfloat16)
        for block in merge_blocks
    ]
    query_grads, key_grads, value_grads = attend_back(
        cross_queries, cross_keys, cross_values, next_bias, heads_grads, cross_heads, cross_sums
    )
    query_grads = scaled_grads(query_grads)
    terms = [None] * model_total
    for step in order:
        next_term = back_rows(key_grads[step], cross_weights[1]) + back_rows(
            value_grads[step], cross_weights[2]
        )
        returned = shifted(next_term.astype(jnp.bfloat16), "view", 1).astype(jnp.float32)
        terms[step] = back_rows(query_grads[step], cross_weights[0]) + returned
    cross_norm_grad = own_sum(terms)
    cross_merge_grad = weight_sums(cross_heads, merge_blocks)
    cross_project_grad = jnp.stack(
        [
            weight_sums(cross_blocks, query_grads),
            weight_sums(next_blocks, key_grads),
            weight_sums(next_blocks, value_grads),
        ]
    )
    cross_low = (cross_project_grad.astype(jnp.bfloat16), cross_merge_grad.astype(jnp.bfloat16))
    cross_low, (up_sum, down_sum) = lax.optimization_barrier((cross_low, (up_sum, down_sum)))
    cross_project_sum, cross_merge_sum = lax.psum(cross_low, "dp")
    rows_grad_cross, gain_cross_grad = layer_norm_back(
        cross_norm_grad, unit_cross, inverse_cross, norm_cross[0]
    )
    first_grad = second_grad + rows_grad_cross

    merge_blocks = row_blocks(first_grad.astype(jnp.bfloat16))
    heads_grads = [
        product(block, self_merge[0], "csd,ed->cse").astype(jnp.bfloat16) for block in merge_blocks
    ]
    query_grads, key_grads, value_grads = attend_back(
        self_queries, self_keys, self_values, own_bias, heads_grads, self_heads, self_sums
    )
    query_grads = scaled_grads(query_grads)
    self_norm_grad = own_sum(
        [
            back_rows(query_grads[step], self_weights[0])
            + back_rows(key_grads[step], self_weights[1])
            + back_rows(value_grads[step], self_weights[2])
            for step in range(model_total)
        ]
    )
    self_merge_grad = weight_sums(self_heads, merge_blocks)
    self_project_grad = jnp.stack(
        [
            weight_sums(self_blocks, query_grads),
            weight_sums(self_blocks, key_grads),
            weight_sums(self_blocks, value_grads),
        ]
    )
    self_low = (self_project_grad.astype(jnp.bfloat16), self_merge_grad.astype(jnp.bfloat16))
    self_low, (cross_project_sum, cross_merge_sum) = lax.optimization_barrier(
        (self_low, (cross_project_sum, cross_merge_sum))
    )
    self_project_sum, self_merge_sum = lax.psum(self_low, "dp")
    rows_grad_self, gain_self_grad = layer_norm_back(
        self_norm_grad, unit_self, inverse_self, norm_self[0]
    )
    mixed_grad = first_grad + rows_grad_self
    gains = jnp.stack([gain_self_grad, gain_cross_grad, gain_hidden_grad])
    gains = jnp.sum(trade(gains, ("dp", "mp"), False, 3), 0)

    sent_rows = ((1.0 - mixing) * mixed_grad).astype(jnp.bfloat16)
    clips = jnp.arange(clip_total, dtype=jnp.int32)
    inverse_partner = jnp.sum(
        jnp.where(partner[None, :] == clips[:, None], clips[None, :], 0), 1
    )
    returned_rows = clip_rows(sent_rows, inverse_partner, 4).astype(jnp.float32)
    tokens_grad = (mixing * mixed_grad + returned_rows)[:, None]
    tokens_out = third_rows.astype(jnp.bfloat16)[:, None]
    return (
        tokens_out,
        summary_out,
        tokens_grad,
        self_project_sum.astype(jnp.float32)[None],
        self_merge_sum.astype(jnp.float32)[None],
        cross_project_sum.astype(jnp.float32)[None],
        cross_merge_sum.astype(jnp.float32)[None],
        up_sum.astype(jnp.float32)[None],
        down_sum.astype(jnp.float32)[None],
        gains[0][None],
        gains[1][None],
        gains[2][None],
        summary_project_grad,
        summary_merge_grad,
        summary_up_grad,
        summary_down_grad,
        summary_norm_self_grad,
        summary_norm_hidden_grad,
    )


def solution(mesh):
    in_specs = (
        P("dp", "view", "mp", None),
        P(),
        P("dp"),
        P(),
        P(),
        P("view", None, None, "mp"),
        P("view", "mp", None),
        P("view", None, None, "mp"),
        P("view", "mp", None),
        P("view", None, "mp"),
        P("view", "mp", None),
        P("view", None),
        P("view", None),
        P("view", None),
        P(None, None, "mp"),
        P("mp", None),
        P(None, "mp"),
        P("mp", None),
        P(),
        P(),
        P("dp", "view", "mp", None),
        P(),
    )
    out_specs = (
        P("dp", "view", "mp", None),
        P(),
        P("dp", "view", "mp", None),
        P("view", None, None, "mp"),
        P("view", "mp", None),
        P("view", None, None, "mp"),
        P("view", "mp", None),
        P("view", None, "mp"),
        P("view", "mp", None),
        P("view", None),
        P("view", None),
        P("view", None),
        P(None, None, "mp"),
        P("mp", None),
        P(None, "mp"),
        P("mp", None),
        P(),
        P(),
    )
    return jax.shard_map(shards, mesh=mesh, in_specs=in_specs, out_specs=out_specs, check_vma=False)
```

```python
import functools

import jax
import jax.numpy as jnp
from jax import lax
from jax.experimental import pallas as pl
from jax.experimental.pallas import tpu as pltpu
from jax.sharding import PartitionSpec as P

D = 768
HEAD = 64
MESH = pl.DeviceIdType.MESH


EPS = 1e-05
NEG = -1000000000.0


def shifted(value, axis, steps):
    count = lax.axis_size(axis)
    pairs = [(source, (source + steps) % count) for source in range(count)]
    return lax.ppermute(value, axis, pairs)


def layer_norm(rows, gain):
    center = rows - jnp.mean(rows, -1, keepdims=True)
    inverse = lax.rsqrt(jnp.mean(center * center, -1, keepdims=True) + EPS)
    unit = center * inverse
    return (unit * gain, unit, inverse)


def layer_norm_back(grad_out, unit, inverse, gain):
    gain_grad = jnp.sum(grad_out * unit, axis=tuple(range(grad_out.ndim - 1)))
    scaled = grad_out * gain
    centered = scaled - jnp.mean(scaled, -1, keepdims=True)
    return (inverse * (centered - unit * jnp.mean(scaled * unit, -1, keepdims=True)), gain_grad)


def gelu_exact(values):
    return jax.nn.gelu(values, approximate=False)


def product(left, right, form):
    return jnp.einsum(form, left, right, preferred_element_type=jnp.float32)


def split_heads(rows):
    return rows.reshape(rows.shape[:-1] + (rows.shape[-1] // HEAD, HEAD))


def merge_heads(rows):
    return rows.reshape(rows.shape[:-2] + (rows.shape[-2] * rows.shape[-1],))


def peer_of(axes, index):
    place = {}
    for axis in reversed(axes):
        count = lax.axis_size(axis)
        place[axis] = index % count
        index = index // count
    return place


def flat_index(axes):
    index = 0
    for axis in axes:
        index = index * lax.axis_size(axis) + lax.axis_index(axis)
    return index


def trade_kernel(axes, total, split, source, target, send_sem, recv_sem, own_sem):
    me = flat_index(axes)
    barrier = pltpu.get_barrier_semaphore()
    for step in range(1, total):
        peer = peer_of(axes, (me + step) % total)
        pl.semaphore_signal(barrier, inc=1, device_id=peer, device_id_type=MESH)
    pl.semaphore_wait(barrier, total - 1)

    def piece(index):
        return source.at[index] if split else source

    own = pltpu.make_async_copy(piece(me), target.at[me], own_sem)
    own.start()
    copies = []
    for step in range(1, total):
        to = (me + step) % total
        copies.append(
            pltpu.make_async_remote_copy(
                src_ref=piece(to),
                dst_ref=target.at[me],
                send_sem=send_sem.at[step],
                recv_sem=recv_sem.at[step],
                device_id=peer_of(axes, to),
                device_id_type=MESH,
            )
        )
        copies[-1].start()
    own.wait()
    for copy in copies:
        copy.wait()


def trade(value, axes, split, collective_id):
    total = 1
    for axis in axes:
        total *= lax.axis_size(axis)
    piece = value.shape[1:] if split else value.shape
    return pl.pallas_call(
        functools.partial(trade_kernel, axes, total, split),
        out_shape=jax.ShapeDtypeStruct((total,) + piece, value.dtype),
        in_specs=[pl.BlockSpec(memory_space=pltpu.VMEM)],
        out_specs=pl.BlockSpec(memory_space=pltpu.VMEM),
        scratch_shapes=[
            pltpu.SemaphoreType.DMA((total,)),
            pltpu.SemaphoreType.DMA((total,)),
            pltpu.SemaphoreType.DMA,
        ],
        compiler_params=pltpu.CompilerParams(collective_id=collective_id, has_side_effects=True),
    )(value)


def pick_kernel(wanted_ref, held_ref, out_ref):
    out_ref[...] = held_ref[...]


def pick(held, wanted):
    block = (1,) + held.shape[1:]
    return pl.pallas_call(
        pick_kernel,
        grid_spec=pltpu.PrefetchScalarGridSpec(
            num_scalar_prefetch=1,
            grid=(held.shape[0],),
            in_specs=[pl.BlockSpec(block, lambda i, wanted_ref: (wanted_ref[i], 0, 0))],
            out_specs=pl.BlockSpec(block, lambda i, wanted_ref: (i, 0, 0)),
        ),
        out_shape=jax.ShapeDtypeStruct(held.shape, held.dtype),
    )(wanted, held)


def clip_rows(rows, wanted, collective_id):
    count = lax.axis_size("dp")
    clips, length, width = rows.shape
    pieces = jnp.swapaxes(rows.reshape(clips, count, length // count, width), 0, 1)
    held = trade(pieces, ("dp",), True, collective_id)
    held = held.reshape(count * clips, length // count, width)
    picked = pick(held, wanted)
    back = trade(picked.reshape(pieces.shape), ("dp",), True, collective_id + 1)
    return jnp.swapaxes(back, 0, 1).reshape(rows.shape)


def row_blocks(piece):
    count = lax.axis_size("mp")
    return [piece] + [shifted(piece, "mp", -step) for step in range(1, count)]


def own_sum(parts):
    total = parts[0]
    for step in range(1, len(parts)):
        total = total + shifted(parts[step].astype(jnp.bfloat16), "mp", step).astype(jnp.float32)
    return total


def whole_sum(value):
    parts = jnp.stack(row_blocks(value))
    if parts.shape[0] > 2:
        parts = jnp.roll(parts, lax.axis_index("mp"), 0)
    return jnp.sum(parts, 0)


def far_first(count):
    return list(range(1, count)) + [0]


def attend_block(query_block, key_rows, value_rows, valid):
    scores = jnp.where(valid, product(query_block, key_rows, "cqhe,ckhe->chqk"), NEG)
    highest = jnp.max(scores, -1, keepdims=True)
    raised = jnp.exp(scores - highest)
    totals = jnp.sum(raised, -1, keepdims=True)
    weights = (raised / totals).astype(jnp.bfloat16)
    result = product(weights, value_rows, "chqk,ckhe->cqhe").astype(jnp.bfloat16)
    return (result, highest + jnp.log(totals))


def attend_block_back(query_block, key_rows, value_rows, valid, grad_block, log_sums):
    scores = jnp.where(valid, product(query_block, key_rows, "cqhe,ckhe->chqk"), NEG)
    weights = jnp.exp(scores - log_sums)
    grad_weights = product(grad_block, value_rows, "cqhe,ckhe->chqk")
    grad_scores = (
        weights * (grad_weights - jnp.sum(weights * grad_weights, -1, keepdims=True))
    ).astype(jnp.bfloat16)
    query_grad = product(grad_scores, key_rows, "chqk,ckhe->cqhe").astype(jnp.bfloat16)
    key_grad = product(grad_scores, query_block, "chqk,cqhe->ckhe")
    value_grad = product(weights.astype(jnp.bfloat16), grad_block, "chqk,cqhe->ckhe")
    return (query_grad, key_grad, value_grad)


def joined(left, right, left_dim, right_dim):
    return lax.dot_general(
        left, right, (((left_dim,), (right_dim,)), ((), ())), preferred_element_type=jnp.float32
    )


def wide_bias(bias_ref, start, length, width):
    part = bias_ref[start : start + length, :]
    return jnp.concatenate([part] * (width // part.shape[1]), 1)


def attend_kernel(parts, chunk, query_ref, *refs):
    key_refs, value_refs = refs[:parts], refs[parts : 2 * parts]
    bias_ref, out_ref, sums_ref = refs[2 * parts :]
    length = key_refs[0].shape[1]
    for half in range(2):
        lanes = slice(HEAD * half, HEAD * half + HEAD)
        keys = [ref[0, :, lanes] for ref in key_refs]
        values = [ref[0, :, lanes] for ref in value_refs]
        for start in range(0, query_ref.shape[1], chunk):
            query = query_ref[0, start : start + chunk, lanes]
            scores = [
                joined(key, query, 1, 1) + wide_bias(bias_ref, j * length, length, chunk)
                for j, key in enumerate(keys)
            ]
            highest = functools.reduce(
                jnp.maximum, [jnp.max(score, 0, keepdims=True) for score in scores]
            )
            raised = [jnp.exp(score - highest) for score in scores]
            totals = sum(jnp.sum(part, 0, keepdims=True) for part in raised)
            result = sum(
                joined(value, part.astype(jnp.bfloat16), 0, 0)
                for value, part in zip(values, raised)
            )
            out_ref[0, start : start + chunk, lanes] = (result / totals).T.astype(jnp.bfloat16)
            sums_ref[0, 0, half : half + 1, start : start + chunk] = highest + jnp.log(totals)


def attend_back_kernel(parts, chunk, first, query_ref, grad_ref, heads_ref, sums_ref, *refs):
    key_refs, value_refs = refs[:parts], refs[parts : 2 * parts]
    bias_ref = refs[2 * parts]
    refs = refs[2 * parts + 1 :]
    held, outs = ((), refs) if first else (refs[: 2 * parts], refs[2 * parts :])
    query_grad_ref, grad_refs = outs[0], outs[1:]
    length = key_refs[0].shape[1]
    for half in range(2):
        lanes = slice(HEAD * half, HEAD * half + HEAD)
        keys = [ref[0, :, lanes] for ref in key_refs]
        values = [ref[0, :, lanes] for ref in value_refs]
        totals = [0.0 if first else ref[0, :, lanes] for ref in held] or [0.0] * (2 * parts)
        for start in range(0, query_ref.shape[1], chunk):
            rows = slice(start, start + chunk)
            query = query_ref[0, rows, lanes]
            grad = grad_ref[0, rows, lanes]
            shared = grad.astype(jnp.float32) * heads_ref[0, rows, lanes].astype(jnp.float32)
            delta = jnp.sum(shared.T, 0, keepdims=True)
            log_sums = sums_ref[0, 0, half : half + 1, rows]
            query_grad = 0.0
            for j in range(parts):
                scores = joined(keys[j], query, 1, 1) + wide_bias(
                    bias_ref, j * length, length, chunk
                )
                weights = jnp.exp(scores - log_sums)
                grad_scores = (weights * (joined(values[j], grad, 1, 1) - delta)).astype(
                    jnp.bfloat16
                )
                totals[j] = totals[j] + joined(grad_scores, query, 1, 0)
                totals[parts + j] = totals[parts + j] + joined(
                    weights.astype(jnp.bfloat16), grad, 1, 0
                )
                query_grad = query_grad + joined(keys[j], grad_scores, 0, 0)
            query_grad_ref[0, rows, lanes] = query_grad.T.astype(jnp.bfloat16)
        for total, ref in zip(totals, grad_refs):
            ref[0, :, lanes] = total.astype(ref.dtype)


def pair_spec(length):
    return pl.BlockSpec((1, length, 2 * HEAD), lambda clip, pair: (clip, 0, pair))


def sums_spec(length):
    return pl.BlockSpec((1, 1, 2, length), lambda clip, pair: (clip, pair, 0, 0))


def bias_spec(length):
    return pl.BlockSpec((length, 2 * HEAD), lambda clip, pair: (0, 0))


CHUNK = 256


def attend(queries, keys, values, bias):
    parts = len(keys)
    clips, length, width = queries[0].shape
    pairs = width // (2 * HEAD)
    heads = [None] * parts
    sums = [None] * parts
    for j in far_first(parts):
        heads[j], sums[j] = pl.pallas_call(
            functools.partial(attend_kernel, parts, min(CHUNK, length)),
            grid=(clips, pairs),
            out_shape=(
                jax.ShapeDtypeStruct((clips, length, width), jnp.bfloat16),
                jax.ShapeDtypeStruct((clips, pairs, 2, length), jnp.float32),
            ),
            in_specs=[pair_spec(length)] * (1 + 2 * parts) + [bias_spec(parts * length)],
            out_specs=(pair_spec(length), sums_spec(length)),
        )(queries[j], *keys, *values, bias)
    return (heads, sums)


def attend_back(queries, keys, values, bias, grads, heads, sums):
    parts = len(keys)
    clips, length, width = queries[0].shape
    pairs = width // (2 * HEAD)
    query_grads = []
    held = []
    for j in range(parts):
        kind = jnp.bfloat16 if j == parts - 1 else jnp.float32
        outs = pl.pallas_call(
            functools.partial(attend_back_kernel, parts, min(CHUNK, length), j == 0),
            grid=(clips, pairs),
            out_shape=[jax.ShapeDtypeStruct((clips, length, width), jnp.bfloat16)]
            + [jax.ShapeDtypeStruct((clips, length, width), kind)] * (2 * parts),
            in_specs=[pair_spec(length)] * 3
            + [sums_spec(length)]
            + [pair_spec(length)] * (2 * parts)
            + [bias_spec(parts * length)]
            + [pair_spec(length)] * len(held),
            out_specs=[pair_spec(length)] * (1 + 2 * parts),
        )(queries[j], grads[j], heads[j], sums[j], *keys, *values, bias, *held)
        query_grads.append(outs[0])
        held = list(outs[1:])
    return (query_grads, held[:parts], held[parts:])


def act_back(before, rows, weight):
    grad = product(rows, weight, "...d,fd->...f")
    return jax.vjp(gelu_exact, before)[1](grad)[0].astype(jnp.bfloat16)


def first_row(blocks, owners):
    row = blocks[0][:, 0]
    for block, owner in zip(blocks[1:], owners[1:]):
        row = jnp.where(owner == 0, block[:, 0], row)
    return row


def clip_ring(rows):
    count = lax.axis_size("dp")
    return jnp.concatenate([rows] + [shifted(rows, "dp", step) for step in range(1, count)])


def with_class(rows, class_rows):
    return (rows.astype(jnp.float32) + class_rows).astype(jnp.bfloat16)


def replaced(left, fresh, stale):
    return product(
        jnp.concatenate([left, -left]), jnp.concatenate([fresh, stale]), "ca,cb->ab"
    )


def project_rows(source, weight):
    return product(source, weight, "csd,de->cse")


def query_rows(source, weight):
    return (project_rows(source, weight) * HEAD ** (-0.5)).astype(jnp.bfloat16)


def back_rows(grad, weight):
    return product(grad, weight, "cse,de->csd")


def weight_sums(sources, grads):
    return sum(product(source, grad, "csd,cse->de") for source, grad in zip(sources, grads))


def scaled_grads(grads):
    return [grad * HEAD ** (-0.5) for grad in grads]


def summary_layer(
    summary_rows, top_grad, weights, gain_top, gain_last, summary_valid
):
    use_project, use_merge, use_up, use_down = weights
    top_normed, top_unit, top_inverse = layer_norm(summary_rows, gain_top)
    top_low = top_normed.astype(jnp.bfloat16)[None]
    top_query = query_rows(top_low, use_project[0])
    top_key = project_rows(top_low, use_project[1]).astype(jnp.bfloat16)
    top_value = project_rows(top_low, use_project[2]).astype(jnp.bfloat16)
    top_key, top_value = split_heads(top_key), split_heads(top_value)
    top_heads, top_sums = attend_block(split_heads(top_query), top_key, top_value, summary_valid)
    top_flat = merge_heads(top_heads)
    summary_mid = summary_rows + whole_sum(product(top_flat, use_merge, "cse,ed->csd")[0])
    mid_normed, mid_unit, mid_inverse = layer_norm(summary_mid, gain_last)
    mid_low = mid_normed.astype(jnp.bfloat16)[None]
    top_before = product(mid_low, use_up, "csd,df->csf")
    top_hidden = gelu_exact(top_before).astype(jnp.bfloat16)
    summary_final = summary_mid + whole_sum(product(top_hidden, use_down, "csf,fd->csd")[0])
    down_input = top_grad.astype(jnp.bfloat16)[None]
    down_grad = product(top_hidden, down_input, "csf,csd->fd")
    act_grad = jax.vjp(gelu_exact, top_before)[1](product(down_input, use_down, "csd,fd->csf"))[
        0
    ].astype(jnp.bfloat16)
    up_grad = product(mid_low, act_grad, "csd,csf->df")
    mid_rows_grad, last_gain_grad = layer_norm_back(
        whole_sum(product(act_grad, use_up, "csf,df->csd")[0]), mid_unit, mid_inverse, gain_last
    )
    mid_grad = top_grad + mid_rows_grad
    merge_input = mid_grad.astype(jnp.bfloat16)[None]
    merge_grad = product(top_flat, merge_input, "cse,csd->ed")
    top_heads_grad = product(merge_input, use_merge, "csd,ed->cse").astype(jnp.bfloat16)
    query_grad, key_grad, value_grad = attend_block_back(
        split_heads(top_query),
        top_key,
        top_value,
        summary_valid,
        split_heads(top_heads_grad),
        top_sums,
    )
    query_grad = merge_heads(query_grad)
    key_grad = merge_heads(key_grad).astype(jnp.bfloat16)
    value_grad = merge_heads(value_grad).astype(jnp.bfloat16)
    query_grad = query_grad * HEAD ** (-0.5)
    project_grad = jnp.stack(
        [product(top_low, grad, "csd,cse->de") for grad in (query_grad, key_grad, value_grad)]
    )
    project_terms = (
        back_rows(query_grad, use_project[0])
        + back_rows(key_grad, use_project[1])
        + back_rows(value_grad, use_project[2])
    )
    first_top_grad, top_gain_grad = layer_norm_back(
        whole_sum(project_terms[0]), top_unit, top_inverse, gain_top
    )
    class_grad = mid_grad + first_top_grad
    return (
        summary_final,
        class_grad,
        (project_grad, merge_grad, up_grad, down_grad),
        top_gain_grad,
        last_gain_grad,
    )


def shards(
    tokens,
    partner,
    mix_weight,
    video_ids,
    view_counts,
    self_project,
    self_merge,
    cross_project,
    cross_merge,
    hidden_up,
    hidden_down,
    norm_self,
    norm_cross,
    norm_hidden,
    summary_project,
    summary_merge,
    summary_up,
    summary_down,
    summary_norm_self,
    summary_norm_hidden,
    tokens_cotangent,
    summary_cotangent,
):
    local_tokens = tokens[:, 0]
    clip_count = local_tokens.shape[0]
    data_index = lax.axis_index("dp")
    view_index = lax.axis_index("view")
    model_index = lax.axis_index("mp")
    view_total = lax.axis_size("view")
    model_total = lax.axis_size("mp")
    clip_total = clip_count * lax.axis_size("dp")
    length = local_tokens.shape[1]
    order = far_first(model_total)
    own_clips = data_index * clip_count + jnp.arange(clip_count, dtype=jnp.int32)
    partner_tokens = clip_rows(local_tokens, partner, 0).astype(jnp.float32)
    grad_blocks = row_blocks(tokens_cotangent[:, 0])
    mixing = mix_weight[:, None, None]
    mixed_rows = mixing * local_tokens.astype(jnp.float32) + (1.0 - mixing) * partner_tokens
    owners = [(model_index + step) % model_total for step in range(model_total)]
    positions = jnp.concatenate([owner * length + jnp.arange(length) for owner in owners])
    own_valid = positions < view_counts[view_index]
    next_valid = positions < view_counts[(view_index + 1) % view_total]
    own_bias, next_bias = (
        jnp.broadcast_to(jnp.where(valid, 0.0, NEG)[:, None], (positions.shape[0], 2 * HEAD))
        for valid in (own_valid, next_valid)
    )

    normed_self, unit_self, inverse_self = layer_norm(mixed_rows, norm_self[0])
    self_blocks = row_blocks(normed_self.astype(jnp.bfloat16))
    self_weights = self_project[0]
    self_queries = [query_rows(block, self_weights[0]) for block in self_blocks]
    self_keys = [project_rows(block, self_weights[1]).astype(jnp.bfloat16) for block in self_blocks]
    self_values = [
        project_rows(block, self_weights[2]).astype(jnp.bfloat16) for block in self_blocks
    ]
    self_heads, self_sums = attend(self_queries, self_keys, self_values, own_bias)
    first_rows = mixed_rows + own_sum(
        [product(heads, self_merge[0], "cse,ed->csd") for heads in self_heads]
    )

    normed_cross, unit_cross, inverse_cross = layer_norm(first_rows, norm_cross[0])
    cross_blocks = row_blocks(normed_cross.astype(jnp.bfloat16))
    next_blocks = [shifted(block, "view", -1) for block in cross_blocks]
    cross_weights = cross_project[0]
    cross_queries = [query_rows(block, cross_weights[0]) for block in cross_blocks]
    cross_keys = [
        project_rows(block, cross_weights[1]).astype(jnp.bfloat16) for block in next_blocks
    ]
    cross_values = [
        project_rows(block, cross_weights[2]).astype(jnp.bfloat16) for block in next_blocks
    ]
    cross_heads, cross_sums = attend(cross_queries, cross_keys, cross_values, next_bias)
    second_rows = first_rows + own_sum(
        [product(heads, cross_merge[0], "cse,ed->csd") for heads in cross_heads]
    )

    normed_hidden, unit_hidden, inverse_hidden = layer_norm(second_rows, norm_hidden[0])
    hidden_blocks = row_blocks(normed_hidden.astype(jnp.bfloat16))
    befores = [product(block, hidden_up[0], "csd,df->csf") for block in hidden_blocks]
    hiddens = [gelu_exact(before).astype(jnp.bfloat16) for before in befores]
    third_rows = second_rows + own_sum(
        [product(hidden, hidden_down[0], "csf,fd->csd") for hidden in hiddens]
    )

    down_rows = grad_blocks
    act_grads = [act_back(before, rows, hidden_down[0]) for before, rows in zip(befores, down_rows)]
    hidden_norm_grad = own_sum(
        [product(act_grad, hidden_up[0], "csf,df->csd") for act_grad in act_grads]
    )
    down_grad = sum(product(h, r, "csf,csd->fd") for h, r in zip(hiddens, down_rows))
    up_grad = sum(product(b, g, "csd,csf->df") for b, g in zip(hidden_blocks, act_grads))
    up_sum, down_sum = lax.psum(
        (up_grad.astype(jnp.bfloat16), down_grad.astype(jnp.bfloat16)), "dp"
    )
    rows_first = [
        first_row(blocks, owners) for blocks in (hidden_blocks, befores, grad_blocks)
    ]
    clip_firsts = [clip_ring(rows) for rows in rows_first]

    everyone = ("dp", "view", "mp")
    class_all = trade(third_rows[:, 0, :], everyone, False, 2)
    class_all = class_all.reshape(clip_total // clip_count, view_total, model_total, clip_count, D)
    class_grid = jnp.swapaxes(class_all[:, :, 0], 1, 2).reshape(clip_total, view_total, D)
    row_total = clip_total * view_total
    token_video = jnp.repeat(video_ids, view_total)
    summary_valid = (token_video[:, None] == token_video[None, :])[None, None]
    summary_final, class_flat, summary_grads, summary_norm_self_grad, summary_norm_hidden_grad = (
        summary_layer(
            class_grid.reshape(row_total, D),
            summary_cotangent.reshape(row_total, D),
            (summary_project, summary_merge, summary_up, summary_down),
            summary_norm_self,
            summary_norm_hidden,
            summary_valid,
        )
    )
    summary_project_grad, summary_merge_grad, summary_up_grad, summary_down_grad = summary_grads
    summary_out = summary_final.reshape(clip_total, view_total, D)
    clip_match = (jnp.arange(clip_total, dtype=jnp.int32)[:, None] == own_clips[None, :]).astype(
        jnp.float32
    )
    view_match = (jnp.arange(view_total) == view_index).astype(jnp.float32)
    class_grad = class_flat.reshape(clip_total, view_total, D)
    view_pick = jnp.sum(class_grad * view_match[None, :, None], axis=1)
    own_class = jnp.sum(clip_match[:, :, None] * view_pick[:, None, :], axis=0)

    first_model = (model_index == 0).astype(jnp.float32)
    third_grad = tokens_cotangent[:, 0].astype(jnp.float32)
    third_grad = third_grad.at[:, 0].add(own_class * first_model)
    true_act = act_back(
        rows_first[1], with_class(rows_first[2], own_class), hidden_down[0]
    )
    true_term = whole_sum(product(true_act, hidden_up[0], "cf,df->cd"))
    hidden_norm_grad = hidden_norm_grad.at[:, 0].set(
        jnp.where(model_index == 0, true_term, hidden_norm_grad[:, 0])
    )
    rows_grad_hidden, gain_hidden_grad = layer_norm_back(
        hidden_norm_grad, unit_hidden, inverse_hidden, norm_hidden[0]
    )
    second_grad = third_grad + rows_grad_hidden

    merge_blocks = row_blocks(second_grad.astype(jnp.bfloat16))
    heads_grads = [
        product(block, cross_merge[0], "csd,ed->cse").astype(jnp.bfloat16)
        for block in merge_blocks
    ]
    query_grads, key_grads, value_grads = attend_back(
        cross_queries, cross_keys, cross_values, next_bias, heads_grads, cross_heads, cross_sums
    )
    query_grads = scaled_grads(query_grads)
    terms = [None] * model_total
    for step in order:
        next_term = back_rows(key_grads[step], cross_weights[1]) + back_rows(
            value_grads[step], cross_weights[2]
        )
        returned = shifted(next_term.astype(jnp.bfloat16), "view", 1).astype(jnp.float32)
        terms[step] = back_rows(query_grads[step], cross_weights[0]) + returned
    cross_norm_grad = own_sum(terms)
    cross_merge_grad = weight_sums(cross_heads, merge_blocks)
    cross_project_grad = jnp.stack(
        [
            weight_sums(cross_blocks, query_grads),
            weight_sums(next_blocks, key_grads),
            weight_sums(next_blocks, value_grads),
        ]
    )
    cross_low = (cross_project_grad.astype(jnp.bfloat16), cross_merge_grad.astype(jnp.bfloat16))
    rows_grad_cross, gain_cross_grad = layer_norm_back(
        cross_norm_grad, unit_cross, inverse_cross, norm_cross[0]
    )
    first_grad = second_grad + rows_grad_cross

    merge_blocks = row_blocks(first_grad.astype(jnp.bfloat16))
    heads_grads = [
        product(block, self_merge[0], "csd,ed->cse").astype(jnp.bfloat16) for block in merge_blocks
    ]
    query_grads, key_grads, value_grads = attend_back(
        self_queries, self_keys, self_values, own_bias, heads_grads, self_heads, self_sums
    )
    query_grads = scaled_grads(query_grads)
    self_norm_grad = own_sum(
        [
            back_rows(query_grads[step], self_weights[0])
            + back_rows(key_grads[step], self_weights[1])
            + back_rows(value_grads[step], self_weights[2])
            for step in range(model_total)
        ]
    )
    self_merge_grad = weight_sums(self_heads, merge_blocks)
    self_project_grad = jnp.stack(
        [
            weight_sums(self_blocks, query_grads),
            weight_sums(self_blocks, key_grads),
            weight_sums(self_blocks, value_grads),
        ]
    )
    self_low = (self_project_grad.astype(jnp.bfloat16), self_merge_grad.astype(jnp.bfloat16))
    self_low, (up_sum, down_sum) = lax.optimization_barrier((self_low, (up_sum, down_sum)))
    (cross_project_sum, cross_merge_sum), (self_project_sum, self_merge_sum) = lax.psum(
        (cross_low, self_low), "dp"
    )
    clip_order = (data_index - jnp.arange(clip_total // clip_count)) % (clip_total // clip_count)
    class_ring = jnp.take(view_pick.reshape(-1, clip_count, D), clip_order, axis=0).reshape(-1, D)
    normed_firsts, before_firsts, raw_firsts = clip_firsts
    true_firsts = with_class(raw_firsts, class_ring)
    hidden_firsts = gelu_exact(before_firsts).astype(jnp.bfloat16)
    down_sum = down_sum.astype(jnp.float32) + replaced(
        hidden_firsts, true_firsts, raw_firsts
    )
    up_sum = up_sum.astype(jnp.float32) + replaced(
        normed_firsts,
        act_back(before_firsts, true_firsts, hidden_down[0]),
        act_back(before_firsts, raw_firsts, hidden_down[0]),
    )
    rows_grad_self, gain_self_grad = layer_norm_back(
        self_norm_grad, unit_self, inverse_self, norm_self[0]
    )
    mixed_grad = first_grad + rows_grad_self
    gains = jnp.stack([gain_self_grad, gain_cross_grad, gain_hidden_grad])
    gains = jnp.sum(trade(gains, ("dp", "mp"), False, 3), 0)

    sent_rows = ((1.0 - mixing) * mixed_grad).astype(jnp.bfloat16)
    clips = jnp.arange(clip_total, dtype=jnp.int32)
    inverse_partner = jnp.sum(
        jnp.where(partner[None, :] == clips[:, None], clips[None, :], 0), 1
    )
    returned_rows = clip_rows(sent_rows, inverse_partner, 4).astype(jnp.float32)
    tokens_grad = (mixing * mixed_grad + returned_rows)[:, None]
    tokens_out = third_rows.astype(jnp.bfloat16)[:, None]
    return (
        tokens_out,
        summary_out,
        tokens_grad,
        self_project_sum.astype(jnp.float32)[None],
        self_merge_sum.astype(jnp.float32)[None],
        cross_project_sum.astype(jnp.float32)[None],
        cross_merge_sum.astype(jnp.float32)[None],
        up_sum[None],
        down_sum[None],
        gains[0][None],
        gains[1][None],
        gains[2][None],
        summary_project_grad,
        summary_merge_grad,
        summary_up_grad,
        summary_down_grad,
        summary_norm_self_grad,
        summary_norm_hidden_grad,
    )


def solution(mesh):
    in_specs = (
        P("dp", "view", "mp", None),
        P(),
        P("dp"),
        P(),
        P(),
        P("view", None, None, "mp"),
        P("view", "mp", None),
        P("view", None, None, "mp"),
        P("view", "mp", None),
        P("view", None, "mp"),
        P("view", "mp", None),
        P("view", None),
        P("view", None),
        P("view", None),
        P(None, None, "mp"),
        P("mp", None),
        P(None, "mp"),
        P("mp", None),
        P(),
        P(),
        P("dp", "view", "mp", None),
        P(),
    )
    out_specs = (
        P("dp", "view", "mp", None),
        P(),
        P("dp", "view", "mp", None),
        P("view", None, None, "mp"),
        P("view", "mp", None),
        P("view", None, None, "mp"),
        P("view", "mp", None),
        P("view", None, "mp"),
        P("view", "mp", None),
        P("view", None),
        P("view", None),
        P("view", None),
        P(None, None, "mp"),
        P("mp", None),
        P(None, "mp"),
        P("mp", None),
        P(),
        P(),
    )
    return jax.shard_map(shards, mesh=mesh, in_specs=in_specs, out_specs=out_specs, check_vma=False)
```

```python
import functools

import jax
import jax.numpy as jnp
from jax import lax
from jax.experimental import pallas as pl
from jax.experimental.pallas import tpu as pltpu
from jax.sharding import PartitionSpec as P

D = 768
HEAD = 64
MESH = pl.DeviceIdType.MESH


EPS = 1e-05
NEG = -1000000000.0


def shifted(value, axis, steps):
    count = lax.axis_size(axis)
    pairs = [(source, (source + steps) % count) for source in range(count)]
    return lax.ppermute(value, axis, pairs)


def layer_norm(rows, gain):
    center = rows - jnp.mean(rows, -1, keepdims=True)
    inverse = lax.rsqrt(jnp.mean(center * center, -1, keepdims=True) + EPS)
    unit = center * inverse
    return (unit * gain, unit, inverse)


def layer_norm_back(grad_out, unit, inverse, gain):
    gain_grad = jnp.sum(grad_out * unit, axis=tuple(range(grad_out.ndim - 1)))
    scaled = grad_out * gain
    centered = scaled - jnp.mean(scaled, -1, keepdims=True)
    return (inverse * (centered - unit * jnp.mean(scaled * unit, -1, keepdims=True)), gain_grad)


def gelu_exact(values):
    return jax.nn.gelu(values, approximate=False)


def product(left, right, form):
    return jnp.einsum(form, left, right, preferred_element_type=jnp.float32)


def split_heads(rows):
    return rows.reshape(rows.shape[:-1] + (rows.shape[-1] // HEAD, HEAD))


def merge_heads(rows):
    return rows.reshape(rows.shape[:-2] + (rows.shape[-2] * rows.shape[-1],))


def peer_of(axes, index):
    place = {}
    for axis in reversed(axes):
        count = lax.axis_size(axis)
        place[axis] = index % count
        index = index // count
    return place


def flat_index(axes):
    index = 0
    for axis in axes:
        index = index * lax.axis_size(axis) + lax.axis_index(axis)
    return index


def trade_kernel(axes, total, split, source, target, send_sem, recv_sem, own_sem):
    me = flat_index(axes)
    barrier = pltpu.get_barrier_semaphore()
    for step in range(1, total):
        peer = peer_of(axes, (me + step) % total)
        pl.semaphore_signal(barrier, inc=1, device_id=peer, device_id_type=MESH)
    pl.semaphore_wait(barrier, total - 1)

    def piece(index):
        return source.at[index] if split else source

    own = pltpu.make_async_copy(piece(me), target.at[me], own_sem)
    own.start()
    copies = []
    for step in range(1, total):
        to = (me + step) % total
        copies.append(
            pltpu.make_async_remote_copy(
                src_ref=piece(to),
                dst_ref=target.at[me],
                send_sem=send_sem.at[step],
                recv_sem=recv_sem.at[step],
                device_id=peer_of(axes, to),
                device_id_type=MESH,
            )
        )
        copies[-1].start()
    own.wait()
    for copy in copies:
        copy.wait()


def trade(value, axes, split, collective_id):
    total = 1
    for axis in axes:
        total *= lax.axis_size(axis)
    piece = value.shape[1:] if split else value.shape
    return pl.pallas_call(
        functools.partial(trade_kernel, axes, total, split),
        out_shape=jax.ShapeDtypeStruct((total,) + piece, value.dtype),
        in_specs=[pl.BlockSpec(memory_space=pltpu.VMEM)],
        out_specs=pl.BlockSpec(memory_space=pltpu.VMEM),
        scratch_shapes=[
            pltpu.SemaphoreType.DMA((total,)),
            pltpu.SemaphoreType.DMA((total,)),
            pltpu.SemaphoreType.DMA,
        ],
        compiler_params=pltpu.CompilerParams(collective_id=collective_id, has_side_effects=True),
    )(value)


def pick_kernel(wanted_ref, held_ref, out_ref):
    out_ref[...] = held_ref[...]


def pick(held, wanted):
    block = (1,) + held.shape[1:]
    return pl.pallas_call(
        pick_kernel,
        grid_spec=pltpu.PrefetchScalarGridSpec(
            num_scalar_prefetch=1,
            grid=(held.shape[0],),
            in_specs=[pl.BlockSpec(block, lambda i, wanted_ref: (wanted_ref[i], 0, 0))],
            out_specs=pl.BlockSpec(block, lambda i, wanted_ref: (i, 0, 0)),
        ),
        out_shape=jax.ShapeDtypeStruct(held.shape, held.dtype),
    )(wanted, held)


def clip_rows(rows, wanted, collective_id):
    count = lax.axis_size("dp")
    clips, length, width = rows.shape
    pieces = jnp.swapaxes(rows.reshape(clips, count, length // count, width), 0, 1)
    held = trade(pieces, ("dp",), True, collective_id)
    held = held.reshape(count * clips, length // count, width)
    picked = pick(held, wanted)
    back = trade(picked.reshape(pieces.shape), ("dp",), True, collective_id + 1)
    return jnp.swapaxes(back, 0, 1).reshape(rows.shape)


def row_blocks(piece):
    count = lax.axis_size("mp")
    return [piece] + [shifted(piece, "mp", -step) for step in range(1, count)]


def own_sum(parts):
    total = parts[0]
    for step in range(1, len(parts)):
        total = total + shifted(parts[step].astype(jnp.bfloat16), "mp", step).astype(jnp.float32)
    return total


def whole_sum(value):
    parts = jnp.stack(row_blocks(value))
    if parts.shape[0] > 2:
        parts = jnp.roll(parts, lax.axis_index("mp"), 0)
    return jnp.sum(parts, 0)


def far_first(count):
    return list(range(1, count)) + [0]


def attend_block(query_block, key_rows, value_rows, valid):
    scores = jnp.where(valid, product(query_block, key_rows, "cqhe,ckhe->chqk"), NEG)
    highest = jnp.max(scores, -1, keepdims=True)
    raised = jnp.exp(scores - highest)
    totals = jnp.sum(raised, -1, keepdims=True)
    weights = (raised / totals).astype(jnp.bfloat16)
    result = product(weights, value_rows, "chqk,ckhe->cqhe").astype(jnp.bfloat16)
    return (result, highest + jnp.log(totals))


def attend_block_back(query_block, key_rows, value_rows, valid, grad_block, log_sums):
    scores = jnp.where(valid, product(query_block, key_rows, "cqhe,ckhe->chqk"), NEG)
    weights = jnp.exp(scores - log_sums)
    grad_weights = product(grad_block, value_rows, "cqhe,ckhe->chqk")
    grad_scores = (
        weights * (grad_weights - jnp.sum(weights * grad_weights, -1, keepdims=True))
    ).astype(jnp.bfloat16)
    query_grad = product(grad_scores, key_rows, "chqk,ckhe->cqhe").astype(jnp.bfloat16)
    key_grad = product(grad_scores, query_block, "chqk,cqhe->ckhe")
    value_grad = product(weights.astype(jnp.bfloat16), grad_block, "chqk,cqhe->ckhe")
    return (query_grad, key_grad, value_grad)


def joined(left, right, left_dim, right_dim):
    return lax.dot_general(
        left, right, (((left_dim,), (right_dim,)), ((), ())), preferred_element_type=jnp.float32
    )


def wide_bias(bias_ref, start, length, width):
    part = bias_ref[start : start + length, :]
    return jnp.concatenate([part] * (width // part.shape[1]), 1)


def attend_kernel(parts, chunk, query_ref, *refs):
    key_refs, value_refs = refs[:parts], refs[parts : 2 * parts]
    bias_ref, out_ref, sums_ref = refs[2 * parts :]
    length = key_refs[0].shape[1]
    for half in range(2):
        lanes = slice(HEAD * half, HEAD * half + HEAD)
        keys = [ref[0, :, lanes] for ref in key_refs]
        values = [ref[0, :, lanes] for ref in value_refs]
        for start in range(0, query_ref.shape[1], chunk):
            query = query_ref[0, start : start + chunk, lanes]
            scores = [
                joined(key, query, 1, 1) + wide_bias(bias_ref, j * length, length, chunk)
                for j, key in enumerate(keys)
            ]
            highest = functools.reduce(
                jnp.maximum, [jnp.max(score, 0, keepdims=True) for score in scores]
            )
            raised = [jnp.exp(score - highest) for score in scores]
            totals = sum(jnp.sum(part, 0, keepdims=True) for part in raised)
            result = sum(
                joined(value, part.astype(jnp.bfloat16), 0, 0)
                for value, part in zip(values, raised)
            )
            out_ref[0, start : start + chunk, lanes] = (result / totals).T.astype(jnp.bfloat16)
            sums_ref[0, 0, half : half + 1, start : start + chunk] = highest + jnp.log(totals)


def attend_back_kernel(parts, chunk, first, query_ref, grad_ref, heads_ref, sums_ref, *refs):
    key_refs, value_refs = refs[:parts], refs[parts : 2 * parts]
    bias_ref = refs[2 * parts]
    refs = refs[2 * parts + 1 :]
    held, outs = ((), refs) if first else (refs[: 2 * parts], refs[2 * parts :])
    query_grad_ref, grad_refs = outs[0], outs[1:]
    length = key_refs[0].shape[1]
    for half in range(2):
        lanes = slice(HEAD * half, HEAD * half + HEAD)
        keys = [ref[0, :, lanes] for ref in key_refs]
        values = [ref[0, :, lanes] for ref in value_refs]
        totals = [0.0 if first else ref[0, :, lanes] for ref in held] or [0.0] * (2 * parts)
        for start in range(0, query_ref.shape[1], chunk):
            rows = slice(start, start + chunk)
            query = query_ref[0, rows, lanes]
            grad = grad_ref[0, rows, lanes]
            shared = grad.astype(jnp.float32) * heads_ref[0, rows, lanes].astype(jnp.float32)
            delta = jnp.sum(shared.T, 0, keepdims=True)
            log_sums = sums_ref[0, 0, half : half + 1, rows]
            query_grad = 0.0
            for j in range(parts):
                scores = joined(keys[j], query, 1, 1) + wide_bias(
                    bias_ref, j * length, length, chunk
                )
                weights = jnp.exp(scores - log_sums)
                grad_scores = (weights * (joined(values[j], grad, 1, 1) - delta)).astype(
                    jnp.bfloat16
                )
                totals[j] = totals[j] + joined(grad_scores, query, 1, 0)
                totals[parts + j] = totals[parts + j] + joined(
                    weights.astype(jnp.bfloat16), grad, 1, 0
                )
                query_grad = query_grad + joined(keys[j], grad_scores, 0, 0)
            query_grad_ref[0, rows, lanes] = query_grad.T.astype(jnp.bfloat16)
        for total, ref in zip(totals, grad_refs):
            ref[0, :, lanes] = total.astype(ref.dtype)


def pair_spec(length):
    return pl.BlockSpec((1, length, 2 * HEAD), lambda clip, pair: (clip, 0, pair))


def sums_spec(length):
    return pl.BlockSpec((1, 1, 2, length), lambda clip, pair: (clip, pair, 0, 0))


def bias_spec(length):
    return pl.BlockSpec((length, 2 * HEAD), lambda clip, pair: (0, 0))


CHUNK = 512


def piece_count(step, length):
    return 2 if step > 0 and length % CHUNK == 0 else 1


def attend(queries, keys, values, bias):
    parts = len(keys)
    clips, length, width = queries[0].shape
    pairs = width // (2 * HEAD)
    heads = [None] * parts
    sums = [None] * parts
    for j in far_first(parts):
        count = piece_count(j, length)
        rows = length // count
        pieces = [
            pl.pallas_call(
                functools.partial(attend_kernel, parts, min(CHUNK, rows)),
                grid=(clips, pairs),
                out_shape=(
                    jax.ShapeDtypeStruct((clips, rows, width), jnp.bfloat16),
                    jax.ShapeDtypeStruct((clips, pairs, 2, rows), jnp.float32),
                ),
                in_specs=[
                    pl.BlockSpec(
                        (1, rows, 2 * HEAD), lambda clip, pair, place=place: (clip, place, pair)
                    )
                ]
                + [pair_spec(length)] * (2 * parts)
                + [bias_spec(parts * length)],
                out_specs=(pair_spec(rows), sums_spec(rows)),
            )(queries[j], *keys, *values, bias)
            for place in range(count)
        ]
        heads[j] = [piece[0] for piece in pieces]
        sums[j] = jnp.concatenate([piece[1] for piece in pieces], -1)
    return (heads, sums)


def merge_sum(heads, weight):
    total = product(heads[0][0], weight, "cse,ed->csd")
    for step in range(1, len(heads)):
        pieces = [
            shifted(product(piece, weight, "cse,ed->csd").astype(jnp.bfloat16), "mp", step)
            for piece in heads[step]
        ]
        total = total + jnp.concatenate(pieces, 1).astype(jnp.float32)
    return total


def whole_heads(heads):
    return [jnp.concatenate(pieces, 1) for pieces in heads]


def attend_back(queries, keys, values, bias, grads, heads, sums):
    parts = len(keys)
    clips, length, width = queries[0].shape
    pairs = width // (2 * HEAD)
    query_grads = []
    held = []
    for j in range(parts):
        kind = jnp.bfloat16 if j == parts - 1 else jnp.float32
        outs = pl.pallas_call(
            functools.partial(attend_back_kernel, parts, min(CHUNK, length), j == 0),
            grid=(clips, pairs),
            out_shape=[jax.ShapeDtypeStruct((clips, length, width), jnp.bfloat16)]
            + [jax.ShapeDtypeStruct((clips, length, width), kind)] * (2 * parts),
            in_specs=[pair_spec(length)] * 3
            + [sums_spec(length)]
            + [pair_spec(length)] * (2 * parts)
            + [bias_spec(parts * length)]
            + [pair_spec(length)] * len(held),
            out_specs=[pair_spec(length)] * (1 + 2 * parts),
        )(queries[j], grads[j], heads[j], sums[j], *keys, *values, bias, *held)
        query_grads.append(outs[0])
        held = list(outs[1:])
    return (query_grads, held[:parts], held[parts:])


def act_back(before, rows, weight):
    grad = product(rows, weight, "...d,fd->...f")
    return jax.vjp(gelu_exact, before)[1](grad)[0].astype(jnp.bfloat16)


def first_row(blocks, owners):
    row = blocks[0][:, 0]
    for block, owner in zip(blocks[1:], owners[1:]):
        row = jnp.where(owner == 0, block[:, 0], row)
    return row


def with_class(rows, class_rows):
    return (rows.astype(jnp.float32) + class_rows).astype(jnp.bfloat16)


def replaced(left, fresh, stale):
    return product(
        jnp.concatenate([left, -left]), jnp.concatenate([fresh, stale]), "ca,cb->ab"
    )


def project_rows(source, weight):
    return product(source, weight, "csd,de->cse")


def query_rows(source, weight):
    return (project_rows(source, weight) * HEAD ** (-0.5)).astype(jnp.bfloat16)


def back_rows(grad, weight):
    return product(grad, weight, "cse,de->csd")


def weight_sums(sources, grads):
    return sum(product(source, grad, "csd,cse->de") for source, grad in zip(sources, grads))


def scaled_grads(grads):
    return [grad * HEAD ** (-0.5) for grad in grads]


def summary_layer(
    summary_rows, top_grad, weights, gain_top, gain_last, summary_valid
):
    use_project, use_merge, use_up, use_down = weights
    top_normed, top_unit, top_inverse = layer_norm(summary_rows, gain_top)
    top_low = top_normed.astype(jnp.bfloat16)[None]
    top_query = query_rows(top_low, use_project[0])
    top_key = project_rows(top_low, use_project[1]).astype(jnp.bfloat16)
    top_value = project_rows(top_low, use_project[2]).astype(jnp.bfloat16)
    top_key, top_value = split_heads(top_key), split_heads(top_value)
    top_heads, top_sums = attend_block(split_heads(top_query), top_key, top_value, summary_valid)
    top_flat = merge_heads(top_heads)
    summary_mid = summary_rows + whole_sum(product(top_flat, use_merge, "cse,ed->csd")[0])
    mid_normed, mid_unit, mid_inverse = layer_norm(summary_mid, gain_last)
    mid_low = mid_normed.astype(jnp.bfloat16)[None]
    top_before = product(mid_low, use_up, "csd,df->csf")
    top_hidden = gelu_exact(top_before).astype(jnp.bfloat16)
    summary_final = summary_mid + whole_sum(product(top_hidden, use_down, "csf,fd->csd")[0])
    down_input = top_grad.astype(jnp.bfloat16)[None]
    act_grad = jax.vjp(gelu_exact, top_before)[1](product(down_input, use_down, "csd,fd->csf"))[
        0
    ].astype(jnp.bfloat16)
    mid_rows_grad, last_gain_grad = layer_norm_back(
        whole_sum(product(act_grad, use_up, "csf,df->csd")[0]), mid_unit, mid_inverse, gain_last
    )
    mid_grad = top_grad + mid_rows_grad
    merge_input = mid_grad.astype(jnp.bfloat16)[None]
    top_heads_grad = product(merge_input, use_merge, "csd,ed->cse").astype(jnp.bfloat16)
    query_grad, key_grad, value_grad = attend_block_back(
        split_heads(top_query),
        top_key,
        top_value,
        summary_valid,
        split_heads(top_heads_grad),
        top_sums,
    )
    query_grad = merge_heads(query_grad)
    key_grad = merge_heads(key_grad).astype(jnp.bfloat16)
    value_grad = merge_heads(value_grad).astype(jnp.bfloat16)
    query_grad = query_grad * HEAD ** (-0.5)
    project_terms = (
        back_rows(query_grad, use_project[0])
        + back_rows(key_grad, use_project[1])
        + back_rows(value_grad, use_project[2])
    )
    first_top_grad, top_gain_grad = layer_norm_back(
        whole_sum(project_terms[0]), top_unit, top_inverse, gain_top
    )
    class_grad = mid_grad + first_top_grad
    return (
        summary_final,
        class_grad,
        (
            (top_low, query_grad),
            (top_low, key_grad),
            (top_low, value_grad),
            (top_flat, merge_input),
            (mid_low, act_grad),
            (top_hidden, down_input),
        ),
        top_gain_grad,
        last_gain_grad,
    )


def shards(
    tokens,
    partner,
    mix_weight,
    video_ids,
    view_counts,
    self_project,
    self_merge,
    cross_project,
    cross_merge,
    hidden_up,
    hidden_down,
    norm_self,
    norm_cross,
    norm_hidden,
    summary_project,
    summary_merge,
    summary_up,
    summary_down,
    summary_norm_self,
    summary_norm_hidden,
    tokens_cotangent,
    summary_cotangent,
):
    local_tokens = tokens[:, 0]
    clip_count = local_tokens.shape[0]
    data_index = lax.axis_index("dp")
    view_index = lax.axis_index("view")
    model_index = lax.axis_index("mp")
    view_total = lax.axis_size("view")
    model_total = lax.axis_size("mp")
    clip_total = clip_count * lax.axis_size("dp")
    length = local_tokens.shape[1]
    order = far_first(model_total)
    own_clips = data_index * clip_count + jnp.arange(clip_count, dtype=jnp.int32)
    partner_tokens = clip_rows(local_tokens, partner, 0).astype(jnp.float32)
    grad_blocks = row_blocks(tokens_cotangent[:, 0])
    mixing = mix_weight[:, None, None]
    mixed_rows = mixing * local_tokens.astype(jnp.float32) + (1.0 - mixing) * partner_tokens
    owners = [(model_index + step) % model_total for step in range(model_total)]
    positions = jnp.concatenate([owner * length + jnp.arange(length) for owner in owners])
    own_valid = positions < view_counts[view_index]
    next_valid = positions < view_counts[(view_index + 1) % view_total]
    own_bias, next_bias = (
        jnp.broadcast_to(jnp.where(valid, 0.0, NEG)[:, None], (positions.shape[0], 2 * HEAD))
        for valid in (own_valid, next_valid)
    )

    normed_self, unit_self, inverse_self = layer_norm(mixed_rows, norm_self[0])
    self_blocks = row_blocks(normed_self.astype(jnp.bfloat16))
    self_weights = self_project[0]
    self_queries = [query_rows(block, self_weights[0]) for block in self_blocks]
    self_keys = [project_rows(block, self_weights[1]).astype(jnp.bfloat16) for block in self_blocks]
    self_values = [
        project_rows(block, self_weights[2]).astype(jnp.bfloat16) for block in self_blocks
    ]
    self_heads, self_sums = attend(self_queries, self_keys, self_values, own_bias)
    first_rows = mixed_rows + merge_sum(self_heads, self_merge[0])
    self_heads = whole_heads(self_heads)

    normed_cross, unit_cross, inverse_cross = layer_norm(first_rows, norm_cross[0])
    cross_blocks = row_blocks(normed_cross.astype(jnp.bfloat16))
    next_blocks = [shifted(block, "view", -1) for block in cross_blocks]
    cross_weights = cross_project[0]
    cross_queries = [query_rows(block, cross_weights[0]) for block in cross_blocks]
    cross_keys = [
        project_rows(block, cross_weights[1]).astype(jnp.bfloat16) for block in next_blocks
    ]
    cross_values = [
        project_rows(block, cross_weights[2]).astype(jnp.bfloat16) for block in next_blocks
    ]
    cross_heads, cross_sums = attend(cross_queries, cross_keys, cross_values, next_bias)
    second_rows = first_rows + merge_sum(cross_heads, cross_merge[0])
    cross_heads = whole_heads(cross_heads)

    normed_hidden, unit_hidden, inverse_hidden = layer_norm(second_rows, norm_hidden[0])
    hidden_blocks = row_blocks(normed_hidden.astype(jnp.bfloat16))
    normed_first = first_row(hidden_blocks, owners)
    before_first = product(normed_first, hidden_up[0], "cd,df->cf")
    raw_first = first_row(grad_blocks, owners)
    class_term = whole_sum(
        product(gelu_exact(before_first).astype(jnp.bfloat16), hidden_down[0], "cf,fd->cd")
    )
    befores = [product(block, hidden_up[0], "csd,df->csf") for block in hidden_blocks]
    hiddens = [gelu_exact(before).astype(jnp.bfloat16) for before in befores]
    third_rows = second_rows + own_sum(
        [product(hidden, hidden_down[0], "csf,fd->csd") for hidden in hiddens]
    )

    down_rows = grad_blocks
    act_grads = [act_back(before, rows, hidden_down[0]) for before, rows in zip(befores, down_rows)]
    hidden_norm_grad = own_sum(
        [product(act_grad, hidden_up[0], "csf,df->csd") for act_grad in act_grads]
    )
    down_grad = sum(product(h, r, "csf,csd->fd") for h, r in zip(hiddens, down_rows))
    up_grad = sum(product(b, g, "csd,csf->df") for b, g in zip(hidden_blocks, act_grads))
    up_sum, down_sum = lax.psum(
        (up_grad.astype(jnp.bfloat16), down_grad.astype(jnp.bfloat16)), "dp"
    )
    everyone = ("dp", "view", "mp")
    class_all = trade(second_rows[:, 0] + class_term, everyone, False, 2)
    class_all = class_all.reshape(clip_total // clip_count, view_total, model_total, clip_count, D)
    class_grid = jnp.swapaxes(class_all[:, :, 0], 1, 2).reshape(clip_total, view_total, D)
    row_total = clip_total * view_total
    token_video = jnp.repeat(video_ids, view_total)
    summary_valid = (token_video[:, None] == token_video[None, :])[None, None]
    summary_final, class_flat, summary_pairs, summary_norm_self_grad, summary_norm_hidden_grad = (
        summary_layer(
            class_grid.reshape(row_total, D),
            summary_cotangent.reshape(row_total, D),
            (summary_project, summary_merge, summary_up, summary_down),
            summary_norm_self,
            summary_norm_hidden,
            summary_valid,
        )
    )
    summary_out = summary_final.reshape(clip_total, view_total, D)
    clip_match = (jnp.arange(clip_total, dtype=jnp.int32)[:, None] == own_clips[None, :]).astype(
        jnp.float32
    )
    view_match = (jnp.arange(view_total) == view_index).astype(jnp.float32)
    class_grad = class_flat.reshape(clip_total, view_total, D)
    view_pick = jnp.sum(class_grad * view_match[None, :, None], axis=1)
    own_class = jnp.sum(clip_match[:, :, None] * view_pick[:, None, :], axis=0)

    first_model = (model_index == 0).astype(jnp.float32)
    third_grad = tokens_cotangent[:, 0].astype(jnp.float32)
    third_grad = third_grad.at[:, 0].add(own_class * first_model)
    true_act = act_back(before_first, with_class(raw_first, own_class), hidden_down[0])
    true_term = whole_sum(product(true_act, hidden_up[0], "cf,df->cd"))
    hidden_norm_grad = hidden_norm_grad.at[:, 0].set(
        jnp.where(model_index == 0, true_term, hidden_norm_grad[:, 0])
    )
    rows_grad_hidden, gain_hidden_grad = layer_norm_back(
        hidden_norm_grad, unit_hidden, inverse_hidden, norm_hidden[0]
    )
    second_grad = third_grad + rows_grad_hidden

    merge_blocks = row_blocks(second_grad.astype(jnp.bfloat16))
    heads_grads = [
        product(block, cross_merge[0], "csd,ed->cse").astype(jnp.bfloat16)
        for block in merge_blocks
    ]
    query_grads, key_grads, value_grads = attend_back(
        cross_queries, cross_keys, cross_values, next_bias, heads_grads, cross_heads, cross_sums
    )
    query_grads = scaled_grads(query_grads)
    terms = [None] * model_total
    for step in order:
        next_term = back_rows(key_grads[step], cross_weights[1]) + back_rows(
            value_grads[step], cross_weights[2]
        )
        returned = shifted(next_term.astype(jnp.bfloat16), "view", 1).astype(jnp.float32)
        terms[step] = back_rows(query_grads[step], cross_weights[0]) + returned
    cross_norm_grad = own_sum(terms)
    cross_merge_grad = weight_sums(cross_heads, merge_blocks)
    cross_project_grad = jnp.stack(
        [
            weight_sums(cross_blocks, query_grads),
            weight_sums(next_blocks, key_grads),
            weight_sums(next_blocks, value_grads),
        ]
    )
    cross_low = (cross_project_grad.astype(jnp.bfloat16), cross_merge_grad.astype(jnp.bfloat16))
    rows_grad_cross, gain_cross_grad = layer_norm_back(
        cross_norm_grad, unit_cross, inverse_cross, norm_cross[0]
    )
    first_grad = second_grad + rows_grad_cross

    merge_blocks = row_blocks(first_grad.astype(jnp.bfloat16))
    heads_grads = [
        product(block, self_merge[0], "csd,ed->cse").astype(jnp.bfloat16) for block in merge_blocks
    ]
    query_grads, key_grads, value_grads = attend_back(
        self_queries, self_keys, self_values, own_bias, heads_grads, self_heads, self_sums
    )
    query_grads = scaled_grads(query_grads)
    self_norm_grad = own_sum(
        [
            back_rows(query_grads[step], self_weights[0])
            + back_rows(key_grads[step], self_weights[1])
            + back_rows(value_grads[step], self_weights[2])
            for step in range(model_total)
        ]
    )
    self_merge_grad = weight_sums(self_heads, merge_blocks)
    self_project_grad = jnp.stack(
        [
            weight_sums(self_blocks, query_grads),
            weight_sums(self_blocks, key_grads),
            weight_sums(self_blocks, value_grads),
        ]
    )
    self_low = (self_project_grad.astype(jnp.bfloat16), self_merge_grad.astype(jnp.bfloat16))
    self_low, (up_sum, down_sum) = lax.optimization_barrier((self_low, (up_sum, down_sum)))
    (cross_project_sum, cross_merge_sum), (self_project_sum, self_merge_sum) = lax.psum(
        (cross_low, self_low), "dp"
    )
    rows_grad_self, gain_self_grad = layer_norm_back(
        self_norm_grad, unit_self, inverse_self, norm_self[0]
    )
    mixed_grad = first_grad + rows_grad_self
    summary_pairs, mixed_grad = lax.optimization_barrier((summary_pairs, mixed_grad))
    summary_grads = [product(left, right, "csd,cse->de") for left, right in summary_pairs]
    summary_project_grad = jnp.stack(summary_grads[:3])
    summary_merge_grad, summary_up_grad, summary_down_grad = summary_grads[3:]
    gains = jnp.stack([gain_self_grad, gain_cross_grad, gain_hidden_grad])
    firsts = jnp.concatenate(
        [normed_first.astype(jnp.float32), raw_first.astype(jnp.float32), before_first], 1
    ).reshape(-1, D)
    shared = trade(jnp.concatenate([gains, firsts]), ("dp", "mp"), False, 3)
    gains = jnp.sum(shared[:, :3], 0)
    clip_firsts = shared.reshape((-1, model_total) + shared.shape[1:])
    clip_firsts = lax.dynamic_index_in_dim(clip_firsts, model_index, 1, False)[:, 3:]
    clip_firsts = clip_firsts.reshape(clip_total, -1)
    normed_firsts = clip_firsts[:, :D].astype(jnp.bfloat16)
    raw_firsts = clip_firsts[:, D : 2 * D].astype(jnp.bfloat16)
    before_firsts = clip_firsts[:, 2 * D :]
    true_firsts = with_class(raw_firsts, view_pick)
    hidden_firsts = gelu_exact(before_firsts).astype(jnp.bfloat16)
    down_sum = down_sum.astype(jnp.float32) + replaced(
        hidden_firsts, true_firsts, raw_firsts
    )
    up_sum = up_sum.astype(jnp.float32) + replaced(
        normed_firsts,
        act_back(before_firsts, true_firsts, hidden_down[0]),
        act_back(before_firsts, raw_firsts, hidden_down[0]),
    )

    sent_rows = ((1.0 - mixing) * mixed_grad).astype(jnp.bfloat16)
    clips = jnp.arange(clip_total, dtype=jnp.int32)
    inverse_partner = jnp.sum(
        jnp.where(partner[None, :] == clips[:, None], clips[None, :], 0), 1
    )
    returned_rows = clip_rows(sent_rows, inverse_partner, 4).astype(jnp.float32)
    tokens_grad = (mixing * mixed_grad + returned_rows)[:, None]
    tokens_out = third_rows.astype(jnp.bfloat16)[:, None]
    return (
        tokens_out,
        summary_out,
        tokens_grad,
        self_project_sum.astype(jnp.float32)[None],
        self_merge_sum.astype(jnp.float32)[None],
        cross_project_sum.astype(jnp.float32)[None],
        cross_merge_sum.astype(jnp.float32)[None],
        up_sum[None],
        down_sum[None],
        gains[0][None],
        gains[1][None],
        gains[2][None],
        summary_project_grad,
        summary_merge_grad,
        summary_up_grad,
        summary_down_grad,
        summary_norm_self_grad,
        summary_norm_hidden_grad,
    )


def solution(mesh):
    in_specs = (
        P("dp", "view", "mp", None),
        P(),
        P("dp"),
        P(),
        P(),
        P("view", None, None, "mp"),
        P("view", "mp", None),
        P("view", None, None, "mp"),
        P("view", "mp", None),
        P("view", None, "mp"),
        P("view", "mp", None),
        P("view", None),
        P("view", None),
        P("view", None),
        P(None, None, "mp"),
        P("mp", None),
        P(None, "mp"),
        P("mp", None),
        P(),
        P(),
        P("dp", "view", "mp", None),
        P(),
    )
    out_specs = (
        P("dp", "view", "mp", None),
        P(),
        P("dp", "view", "mp", None),
        P("view", None, None, "mp"),
        P("view", "mp", None),
        P("view", None, None, "mp"),
        P("view", "mp", None),
        P("view", None, "mp"),
        P("view", "mp", None),
        P("view", None),
        P("view", None),
        P("view", None),
        P(None, None, "mp"),
        P("mp", None),
        P(None, "mp"),
        P("mp", None),
        P(),
        P(),
    )
    return jax.shard_map(shards, mesh=mesh, in_specs=in_specs, out_specs=out_specs, check_vma=False)
```

```python
import functools

import jax
import jax.numpy as jnp
from jax import lax
from jax.experimental import pallas as pl
from jax.experimental.pallas import tpu as pltpu
from jax.sharding import PartitionSpec as P

D = 768
HEAD = 64
MESH = pl.DeviceIdType.MESH


EPS = 1e-05
NEG = -1000000000.0


def shifted(value, axis, steps):
    count = lax.axis_size(axis)
    pairs = [(source, (source + steps) % count) for source in range(count)]
    return lax.ppermute(value, axis, pairs)


def layer_norm(rows, gain):
    center = rows - jnp.mean(rows, -1, keepdims=True)
    inverse = lax.rsqrt(jnp.mean(center * center, -1, keepdims=True) + EPS)
    unit = center * inverse
    return (unit * gain, unit, inverse)


def layer_norm_back(grad_out, unit, inverse, gain):
    gain_grad = jnp.sum(grad_out * unit, axis=tuple(range(grad_out.ndim - 1)))
    scaled = grad_out * gain
    centered = scaled - jnp.mean(scaled, -1, keepdims=True)
    return (inverse * (centered - unit * jnp.mean(scaled * unit, -1, keepdims=True)), gain_grad)


def gelu_exact(values):
    return jax.nn.gelu(values, approximate=False)


def product(left, right, form):
    return jnp.einsum(form, left, right, preferred_element_type=jnp.float32)


def split_heads(rows):
    return rows.reshape(rows.shape[:-1] + (rows.shape[-1] // HEAD, HEAD))


def merge_heads(rows):
    return rows.reshape(rows.shape[:-2] + (rows.shape[-2] * rows.shape[-1],))


def peer_of(axes, index):
    place = {}
    for axis in reversed(axes):
        count = lax.axis_size(axis)
        place[axis] = index % count
        index = index // count
    return place


def flat_index(axes):
    index = 0
    for axis in axes:
        index = index * lax.axis_size(axis) + lax.axis_index(axis)
    return index


def trade_kernel(axes, total, split, source, target, send_sem, recv_sem, own_sem):
    me = flat_index(axes)
    barrier = pltpu.get_barrier_semaphore()
    for step in range(1, total):
        peer = peer_of(axes, (me + step) % total)
        pl.semaphore_signal(barrier, inc=1, device_id=peer, device_id_type=MESH)
    pl.semaphore_wait(barrier, total - 1)

    def piece(index):
        return source.at[index] if split else source

    own = pltpu.make_async_copy(piece(me), target.at[me], own_sem)
    own.start()
    copies = []
    for step in range(1, total):
        to = (me + step) % total
        copies.append(
            pltpu.make_async_remote_copy(
                src_ref=piece(to),
                dst_ref=target.at[me],
                send_sem=send_sem.at[step],
                recv_sem=recv_sem.at[step],
                device_id=peer_of(axes, to),
                device_id_type=MESH,
            )
        )
        copies[-1].start()
    own.wait()
    for copy in copies:
        copy.wait()


def trade(value, axes, split, collective_id):
    total = 1
    for axis in axes:
        total *= lax.axis_size(axis)
    piece = value.shape[1:] if split else value.shape
    return pl.pallas_call(
        functools.partial(trade_kernel, axes, total, split),
        out_shape=jax.ShapeDtypeStruct((total,) + piece, value.dtype),
        in_specs=[pl.BlockSpec(memory_space=pltpu.VMEM)],
        out_specs=pl.BlockSpec(memory_space=pltpu.VMEM),
        scratch_shapes=[
            pltpu.SemaphoreType.DMA((total,)),
            pltpu.SemaphoreType.DMA((total,)),
            pltpu.SemaphoreType.DMA,
        ],
        compiler_params=pltpu.CompilerParams(collective_id=collective_id, has_side_effects=True),
    )(value)


def pick_kernel(wanted_ref, held_ref, out_ref):
    out_ref[...] = held_ref[...]


def pick(held, wanted):
    block = (1,) + held.shape[1:]
    return pl.pallas_call(
        pick_kernel,
        grid_spec=pltpu.PrefetchScalarGridSpec(
            num_scalar_prefetch=1,
            grid=(held.shape[0],),
            in_specs=[pl.BlockSpec(block, lambda i, wanted_ref: (wanted_ref[i], 0, 0))],
            out_specs=pl.BlockSpec(block, lambda i, wanted_ref: (i, 0, 0)),
        ),
        out_shape=jax.ShapeDtypeStruct(held.shape, held.dtype),
    )(wanted, held)


def clip_rows(rows, wanted, collective_id):
    count = lax.axis_size("dp")
    clips, length, width = rows.shape
    pieces = jnp.swapaxes(rows.reshape(clips, count, length // count, width), 0, 1)
    held = trade(pieces, ("dp",), True, collective_id)
    held = held.reshape(count * clips, length // count, width)
    picked = pick(held, wanted)
    back = trade(picked.reshape(pieces.shape), ("dp",), True, collective_id + 1)
    return jnp.swapaxes(back, 0, 1).reshape(rows.shape)


def row_blocks(piece):
    count = lax.axis_size("mp")
    return [piece] + [shifted(piece, "mp", -step) for step in range(1, count)]


def own_sum(parts):
    total = parts[0]
    for step in range(1, len(parts)):
        total = total + shifted(parts[step].astype(jnp.bfloat16), "mp", step).astype(jnp.float32)
    return total


def whole_sum(value):
    parts = jnp.stack(row_blocks(value))
    if parts.shape[0] > 2:
        parts = jnp.roll(parts, lax.axis_index("mp"), 0)
    return jnp.sum(parts, 0)


def far_first(count):
    return list(range(1, count)) + [0]


def attend_block(query_block, key_rows, value_rows, valid):
    scores = jnp.where(valid, product(query_block, key_rows, "cqhe,ckhe->chqk"), NEG)
    highest = jnp.max(scores, -1, keepdims=True)
    raised = jnp.exp(scores - highest)
    totals = jnp.sum(raised, -1, keepdims=True)
    weights = (raised / totals).astype(jnp.bfloat16)
    result = product(weights, value_rows, "chqk,ckhe->cqhe").astype(jnp.bfloat16)
    return (result, highest + jnp.log(totals))


def attend_block_back(query_block, key_rows, value_rows, valid, grad_block, log_sums):
    scores = jnp.where(valid, product(query_block, key_rows, "cqhe,ckhe->chqk"), NEG)
    weights = jnp.exp(scores - log_sums)
    grad_weights = product(grad_block, value_rows, "cqhe,ckhe->chqk")
    grad_scores = (
        weights * (grad_weights - jnp.sum(weights * grad_weights, -1, keepdims=True))
    ).astype(jnp.bfloat16)
    query_grad = product(grad_scores, key_rows, "chqk,ckhe->cqhe").astype(jnp.bfloat16)
    key_grad = product(grad_scores, query_block, "chqk,cqhe->ckhe")
    value_grad = product(weights.astype(jnp.bfloat16), grad_block, "chqk,cqhe->ckhe")
    return (query_grad, key_grad, value_grad)


def joined(left, right, left_dim, right_dim):
    return lax.dot_general(
        left, right, (((left_dim,), (right_dim,)), ((), ())), preferred_element_type=jnp.float32
    )


def wide_bias(bias_ref, start, length, width):
    part = bias_ref[start : start + length, :]
    return jnp.concatenate([part] * (width // part.shape[1]), 1)


def attend_kernel(parts, chunk, query_ref, *refs):
    key_refs, value_refs = refs[:parts], refs[parts : 2 * parts]
    bias_ref, out_ref, sums_ref = refs[2 * parts :]
    length = key_refs[0].shape[1]
    for half in range(2):
        lanes = slice(HEAD * half, HEAD * half + HEAD)
        keys = [ref[0, :, lanes] for ref in key_refs]
        values = [ref[0, :, lanes] for ref in value_refs]
        for start in range(0, query_ref.shape[1], chunk):
            query = query_ref[0, start : start + chunk, lanes]
            scores = [
                joined(key, query, 1, 1) + wide_bias(bias_ref, j * length, length, chunk)
                for j, key in enumerate(keys)
            ]
            highest = functools.reduce(
                jnp.maximum, [jnp.max(score, 0, keepdims=True) for score in scores]
            )
            raised = [jnp.exp(score - highest) for score in scores]
            totals = sum(jnp.sum(part, 0, keepdims=True) for part in raised)
            result = sum(
                joined(value, part.astype(jnp.bfloat16), 0, 0)
                for value, part in zip(values, raised)
            )
            out_ref[0, start : start + chunk, lanes] = (result / totals).T.astype(jnp.bfloat16)
            sums_ref[0, 0, half : half + 1, start : start + chunk] = highest + jnp.log(totals)


def attend_back_kernel(parts, chunk, first, query_ref, grad_ref, heads_ref, sums_ref, *refs):
    key_refs, value_refs = refs[:parts], refs[parts : 2 * parts]
    bias_ref = refs[2 * parts]
    refs = refs[2 * parts + 1 :]
    held, outs = ((), refs) if first else (refs[: 2 * parts], refs[2 * parts :])
    query_grad_ref, grad_refs = outs[0], outs[1:]
    length = key_refs[0].shape[1]
    for half in range(2):
        lanes = slice(HEAD * half, HEAD * half + HEAD)
        keys = [ref[0, :, lanes] for ref in key_refs]
        values = [ref[0, :, lanes] for ref in value_refs]
        totals = [0.0 if first else ref[0, :, lanes] for ref in held] or [0.0] * (2 * parts)
        for start in range(0, query_ref.shape[1], chunk):
            rows = slice(start, start + chunk)
            query = query_ref[0, rows, lanes]
            grad = grad_ref[0, rows, lanes]
            shared = grad.astype(jnp.float32) * heads_ref[0, rows, lanes].astype(jnp.float32)
            delta = jnp.sum(shared.T, 0, keepdims=True)
            log_sums = sums_ref[0, 0, half : half + 1, rows]
            query_grad = 0.0
            for j in range(parts):
                scores = joined(keys[j], query, 1, 1) + wide_bias(
                    bias_ref, j * length, length, chunk
                )
                weights = jnp.exp(scores - log_sums)
                grad_scores = (weights * (joined(values[j], grad, 1, 1) - delta)).astype(
                    jnp.bfloat16
                )
                totals[j] = totals[j] + joined(grad_scores, query, 1, 0)
                totals[parts + j] = totals[parts + j] + joined(
                    weights.astype(jnp.bfloat16), grad, 1, 0
                )
                query_grad = query_grad + joined(keys[j], grad_scores, 0, 0)
            query_grad_ref[0, rows, lanes] = query_grad.T.astype(jnp.bfloat16)
        for total, ref in zip(totals, grad_refs):
            ref[0, :, lanes] = total.astype(ref.dtype)


def pair_spec(length):
    return pl.BlockSpec((1, length, 2 * HEAD), lambda clip, pair: (clip, 0, pair))


def sums_spec(length):
    return pl.BlockSpec((1, 1, 2, length), lambda clip, pair: (clip, pair, 0, 0))


def bias_spec(length):
    return pl.BlockSpec((length, 2 * HEAD), lambda clip, pair: (0, 0))


CHUNK = 512


def piece_count(step, length):
    return 2 if step > 0 and length % CHUNK == 0 else 1


def attend(queries, keys, values, bias):
    parts = len(keys)
    clips, length, width = queries[0].shape
    pairs = width // (2 * HEAD)
    heads = [None] * parts
    sums = [None] * parts
    for j in far_first(parts):
        count = piece_count(j, length)
        rows = length // count
        pieces = [
            pl.pallas_call(
                functools.partial(attend_kernel, parts, min(CHUNK, rows)),
                grid=(clips, pairs),
                out_shape=(
                    jax.ShapeDtypeStruct((clips, rows, width), jnp.bfloat16),
                    jax.ShapeDtypeStruct((clips, pairs, 2, rows), jnp.float32),
                ),
                in_specs=[
                    pl.BlockSpec(
                        (1, rows, 2 * HEAD), lambda clip, pair, place=place: (clip, place, pair)
                    )
                ]
                + [pair_spec(length)] * (2 * parts)
                + [bias_spec(parts * length)],
                out_specs=(pair_spec(rows), sums_spec(rows)),
            )(queries[j], *keys, *values, bias)
            for place in range(count)
        ]
        heads[j] = [piece[0] for piece in pieces]
        sums[j] = jnp.concatenate([piece[1] for piece in pieces], -1)
    return (heads, sums)


def merge_sum(heads, weight):
    total = product(heads[0][0], weight, "cse,ed->csd")
    for step in range(1, len(heads)):
        pieces = [
            shifted(product(piece, weight, "cse,ed->csd").astype(jnp.bfloat16), "mp", step)
            for piece in heads[step]
        ]
        total = total + jnp.concatenate(pieces, 1).astype(jnp.float32)
    return total


def whole_heads(heads):
    return [jnp.concatenate(pieces, 1) for pieces in heads]


def attend_back(queries, keys, values, bias, grads, heads, sums):
    parts = len(keys)
    clips, length, width = queries[0].shape
    pairs = width // (2 * HEAD)
    query_grads = []
    held = []
    for j in range(parts):
        kind = jnp.bfloat16 if j == parts - 1 else jnp.float32
        outs = pl.pallas_call(
            functools.partial(attend_back_kernel, parts, min(CHUNK, length), j == 0),
            grid=(clips, pairs),
            out_shape=[jax.ShapeDtypeStruct((clips, length, width), jnp.bfloat16)]
            + [jax.ShapeDtypeStruct((clips, length, width), kind)] * (2 * parts),
            in_specs=[pair_spec(length)] * 3
            + [sums_spec(length)]
            + [pair_spec(length)] * (2 * parts)
            + [bias_spec(parts * length)]
            + [pair_spec(length)] * len(held),
            out_specs=[pair_spec(length)] * (1 + 2 * parts),
        )(queries[j], grads[j], heads[j], sums[j], *keys, *values, bias, *held)
        query_grads.append(outs[0])
        held = list(outs[1:])
    return (query_grads, held[:parts], held[parts:])


def pair_swap(value):
    count = lax.axis_size("dp")
    return lax.ppermute(value, "dp", [(i, i ^ 1) for i in range(count)])


def pair_half(value):
    rows = value.reshape(-1, value.shape[-1])
    half = rows.shape[0] // 2
    odd = lax.axis_index("dp") % 2
    kept = lax.dynamic_slice_in_dim(rows, odd * half, half)
    sent = lax.dynamic_slice_in_dim(rows, (1 - odd) * half, half)
    got = pair_swap(sent)
    return (kept.astype(jnp.float32) + got.astype(jnp.float32)).astype(jnp.bfloat16)


def line_sum(halves):
    count = lax.axis_size("dp")
    groups = [list(range(odd, count, 2)) for odd in range(2)]
    return lax.psum(halves, "dp", axis_index_groups=groups)


def pair_whole(half, shape):
    got = pair_swap(half)
    odd = lax.axis_index("dp") % 2
    pieces = jnp.stack([jnp.where(odd == 0, half, got), jnp.where(odd == 0, got, half)])
    return pieces.reshape(shape).astype(jnp.float32)


def act_back(before, rows, weight):
    grad = product(rows, weight, "...d,fd->...f")
    return jax.vjp(gelu_exact, before)[1](grad)[0].astype(jnp.bfloat16)


def first_row(blocks, owners):
    row = blocks[0][:, 0]
    for block, owner in zip(blocks[1:], owners[1:]):
        row = jnp.where(owner == 0, block[:, 0], row)
    return row


def with_class(rows, class_rows):
    return (rows.astype(jnp.float32) + class_rows).astype(jnp.bfloat16)


def replaced(left, fresh, stale):
    return product(
        jnp.concatenate([left, -left]), jnp.concatenate([fresh, stale]), "ca,cb->ab"
    )


def project_rows(source, weight):
    return product(source, weight, "csd,de->cse")


def query_rows(source, weight):
    return (project_rows(source, weight) * HEAD ** (-0.5)).astype(jnp.bfloat16)


def back_rows(grad, weight):
    return product(grad, weight, "cse,de->csd")


def weight_sums(sources, grads):
    return sum(product(source, grad, "csd,cse->de") for source, grad in zip(sources, grads))


def scaled_grads(grads):
    return [grad * HEAD ** (-0.5) for grad in grads]


def summary_layer(
    summary_rows, top_grad, weights, gain_top, gain_last, summary_valid
):
    use_project, use_merge, use_up, use_down = weights
    top_normed, top_unit, top_inverse = layer_norm(summary_rows, gain_top)
    top_low = top_normed.astype(jnp.bfloat16)[None]
    top_query = query_rows(top_low, use_project[0])
    top_key = project_rows(top_low, use_project[1]).astype(jnp.bfloat16)
    top_value = project_rows(top_low, use_project[2]).astype(jnp.bfloat16)
    top_key, top_value = split_heads(top_key), split_heads(top_value)
    top_heads, top_sums = attend_block(split_heads(top_query), top_key, top_value, summary_valid)
    top_flat = merge_heads(top_heads)
    summary_mid = summary_rows + whole_sum(product(top_flat, use_merge, "cse,ed->csd")[0])
    mid_normed, mid_unit, mid_inverse = layer_norm(summary_mid, gain_last)
    mid_low = mid_normed.astype(jnp.bfloat16)[None]
    top_before = product(mid_low, use_up, "csd,df->csf")
    top_hidden = gelu_exact(top_before).astype(jnp.bfloat16)
    summary_final = summary_mid + whole_sum(product(top_hidden, use_down, "csf,fd->csd")[0])
    down_input = top_grad.astype(jnp.bfloat16)[None]
    act_grad = jax.vjp(gelu_exact, top_before)[1](product(down_input, use_down, "csd,fd->csf"))[
        0
    ].astype(jnp.bfloat16)
    mid_rows_grad, last_gain_grad = layer_norm_back(
        whole_sum(product(act_grad, use_up, "csf,df->csd")[0]), mid_unit, mid_inverse, gain_last
    )
    mid_grad = top_grad + mid_rows_grad
    merge_input = mid_grad.astype(jnp.bfloat16)[None]
    top_heads_grad = product(merge_input, use_merge, "csd,ed->cse").astype(jnp.bfloat16)
    query_grad, key_grad, value_grad = attend_block_back(
        split_heads(top_query),
        top_key,
        top_value,
        summary_valid,
        split_heads(top_heads_grad),
        top_sums,
    )
    query_grad = merge_heads(query_grad)
    key_grad = merge_heads(key_grad).astype(jnp.bfloat16)
    value_grad = merge_heads(value_grad).astype(jnp.bfloat16)
    query_grad = query_grad * HEAD ** (-0.5)
    project_terms = (
        back_rows(query_grad, use_project[0])
        + back_rows(key_grad, use_project[1])
        + back_rows(value_grad, use_project[2])
    )
    first_top_grad, top_gain_grad = layer_norm_back(
        whole_sum(project_terms[0]), top_unit, top_inverse, gain_top
    )
    class_grad = mid_grad + first_top_grad
    return (
        summary_final,
        class_grad,
        (
            (top_low, query_grad),
            (top_low, key_grad),
            (top_low, value_grad),
            (top_flat, merge_input),
            (mid_low, act_grad),
            (top_hidden, down_input),
        ),
        top_gain_grad,
        last_gain_grad,
    )


def shards(
    tokens,
    partner,
    mix_weight,
    video_ids,
    view_counts,
    self_project,
    self_merge,
    cross_project,
    cross_merge,
    hidden_up,
    hidden_down,
    norm_self,
    norm_cross,
    norm_hidden,
    summary_project,
    summary_merge,
    summary_up,
    summary_down,
    summary_norm_self,
    summary_norm_hidden,
    tokens_cotangent,
    summary_cotangent,
):
    local_tokens = tokens[:, 0]
    clip_count = local_tokens.shape[0]
    data_index = lax.axis_index("dp")
    view_index = lax.axis_index("view")
    model_index = lax.axis_index("mp")
    view_total = lax.axis_size("view")
    model_total = lax.axis_size("mp")
    clip_total = clip_count * lax.axis_size("dp")
    length = local_tokens.shape[1]
    order = far_first(model_total)
    own_clips = data_index * clip_count + jnp.arange(clip_count, dtype=jnp.int32)
    partner_tokens = clip_rows(local_tokens, partner, 0).astype(jnp.float32)
    grad_blocks = row_blocks(tokens_cotangent[:, 0])
    mixing = mix_weight[:, None, None]
    mixed_rows = mixing * local_tokens.astype(jnp.float32) + (1.0 - mixing) * partner_tokens
    owners = [(model_index + step) % model_total for step in range(model_total)]
    positions = jnp.concatenate([owner * length + jnp.arange(length) for owner in owners])
    own_valid = positions < view_counts[view_index]
    next_valid = positions < view_counts[(view_index + 1) % view_total]
    own_bias, next_bias = (
        jnp.broadcast_to(jnp.where(valid, 0.0, NEG)[:, None], (positions.shape[0], 2 * HEAD))
        for valid in (own_valid, next_valid)
    )

    normed_self, unit_self, inverse_self = layer_norm(mixed_rows, norm_self[0])
    self_blocks = row_blocks(normed_self.astype(jnp.bfloat16))
    self_weights = self_project[0]
    self_queries = [query_rows(block, self_weights[0]) for block in self_blocks]
    self_keys = [project_rows(block, self_weights[1]).astype(jnp.bfloat16) for block in self_blocks]
    self_values = [
        project_rows(block, self_weights[2]).astype(jnp.bfloat16) for block in self_blocks
    ]
    self_heads, self_sums = attend(self_queries, self_keys, self_values, own_bias)
    first_rows = mixed_rows + merge_sum(self_heads, self_merge[0])
    self_heads = whole_heads(self_heads)

    normed_cross, unit_cross, inverse_cross = layer_norm(first_rows, norm_cross[0])
    cross_blocks = row_blocks(normed_cross.astype(jnp.bfloat16))
    next_blocks = [shifted(block, "view", -1) for block in cross_blocks]
    cross_weights = cross_project[0]
    cross_queries = [query_rows(block, cross_weights[0]) for block in cross_blocks]
    cross_keys = [
        project_rows(block, cross_weights[1]).astype(jnp.bfloat16) for block in next_blocks
    ]
    cross_values = [
        project_rows(block, cross_weights[2]).astype(jnp.bfloat16) for block in next_blocks
    ]
    cross_heads, cross_sums = attend(cross_queries, cross_keys, cross_values, next_bias)
    second_rows = first_rows + merge_sum(cross_heads, cross_merge[0])
    cross_heads = whole_heads(cross_heads)

    normed_hidden, unit_hidden, inverse_hidden = layer_norm(second_rows, norm_hidden[0])
    hidden_blocks = row_blocks(normed_hidden.astype(jnp.bfloat16))
    normed_first = first_row(hidden_blocks, owners)
    before_first = product(normed_first, hidden_up[0], "cd,df->cf")
    raw_first = first_row(grad_blocks, owners)
    class_term = whole_sum(
        product(gelu_exact(before_first).astype(jnp.bfloat16), hidden_down[0], "cf,fd->cd")
    )
    befores = [product(block, hidden_up[0], "csd,df->csf") for block in hidden_blocks]
    hiddens = [gelu_exact(before).astype(jnp.bfloat16) for before in befores]
    third_rows = second_rows + own_sum(
        [product(hidden, hidden_down[0], "csf,fd->csd") for hidden in hiddens]
    )

    down_rows = grad_blocks
    act_grads = [act_back(before, rows, hidden_down[0]) for before, rows in zip(befores, down_rows)]
    hidden_norm_grad = own_sum(
        [product(act_grad, hidden_up[0], "csf,df->csd") for act_grad in act_grads]
    )
    down_grad = sum(product(h, r, "csf,csd->fd") for h, r in zip(hiddens, down_rows))
    up_grad = sum(product(b, g, "csd,csf->df") for b, g in zip(hidden_blocks, act_grads))
    up_half = pair_half(up_grad.astype(jnp.bfloat16))
    down_half = pair_half(down_grad.astype(jnp.bfloat16))
    everyone = ("dp", "view", "mp")
    class_all = trade(second_rows[:, 0] + class_term, everyone, False, 2)
    class_all = class_all.reshape(clip_total // clip_count, view_total, model_total, clip_count, D)
    class_grid = jnp.swapaxes(class_all[:, :, 0], 1, 2).reshape(clip_total, view_total, D)
    row_total = clip_total * view_total
    token_video = jnp.repeat(video_ids, view_total)
    summary_valid = (token_video[:, None] == token_video[None, :])[None, None]
    summary_final, class_flat, summary_pairs, summary_norm_self_grad, summary_norm_hidden_grad = (
        summary_layer(
            class_grid.reshape(row_total, D),
            summary_cotangent.reshape(row_total, D),
            (summary_project, summary_merge, summary_up, summary_down),
            summary_norm_self,
            summary_norm_hidden,
            summary_valid,
        )
    )
    summary_out = summary_final.reshape(clip_total, view_total, D)
    clip_match = (jnp.arange(clip_total, dtype=jnp.int32)[:, None] == own_clips[None, :]).astype(
        jnp.float32
    )
    view_match = (jnp.arange(view_total) == view_index).astype(jnp.float32)
    class_grad = class_flat.reshape(clip_total, view_total, D)
    view_pick = jnp.sum(class_grad * view_match[None, :, None], axis=1)
    own_class = jnp.sum(clip_match[:, :, None] * view_pick[:, None, :], axis=0)
    (up_half, down_half), own_class = lax.optimization_barrier(((up_half, down_half), own_class))
    up_half, down_half = line_sum((up_half, down_half))

    first_model = (model_index == 0).astype(jnp.float32)
    third_grad = tokens_cotangent[:, 0].astype(jnp.float32)
    third_grad = third_grad.at[:, 0].add(own_class * first_model)
    true_act = act_back(before_first, with_class(raw_first, own_class), hidden_down[0])
    true_term = whole_sum(product(true_act, hidden_up[0], "cf,df->cd"))
    hidden_norm_grad = hidden_norm_grad.at[:, 0].set(
        jnp.where(model_index == 0, true_term, hidden_norm_grad[:, 0])
    )
    rows_grad_hidden, gain_hidden_grad = layer_norm_back(
        hidden_norm_grad, unit_hidden, inverse_hidden, norm_hidden[0]
    )
    second_grad = third_grad + rows_grad_hidden

    merge_blocks = row_blocks(second_grad.astype(jnp.bfloat16))
    heads_grads = [
        product(block, cross_merge[0], "csd,ed->cse").astype(jnp.bfloat16)
        for block in merge_blocks
    ]
    query_grads, key_grads, value_grads = attend_back(
        cross_queries, cross_keys, cross_values, next_bias, heads_grads, cross_heads, cross_sums
    )
    query_grads = scaled_grads(query_grads)
    terms = [None] * model_total
    for step in order:
        next_term = back_rows(key_grads[step], cross_weights[1]) + back_rows(
            value_grads[step], cross_weights[2]
        )
        returned = shifted(next_term.astype(jnp.bfloat16), "view", 1).astype(jnp.float32)
        terms[step] = back_rows(query_grads[step], cross_weights[0]) + returned
    cross_norm_grad = own_sum(terms)
    cross_merge_grad = weight_sums(cross_heads, merge_blocks)
    cross_project_grad = jnp.stack(
        [
            weight_sums(cross_blocks, query_grads),
            weight_sums(next_blocks, key_grads),
            weight_sums(next_blocks, value_grads),
        ]
    )
    cross_halves = (
        pair_half(cross_project_grad.astype(jnp.bfloat16)),
        pair_half(cross_merge_grad.astype(jnp.bfloat16)),
    )
    rows_grad_cross, gain_cross_grad = layer_norm_back(
        cross_norm_grad, unit_cross, inverse_cross, norm_cross[0]
    )
    first_grad = second_grad + rows_grad_cross

    merge_blocks = row_blocks(first_grad.astype(jnp.bfloat16))
    cross_halves, up_half, down_half, merge_blocks[-1] = lax.optimization_barrier(
        (cross_halves, up_half, down_half, merge_blocks[-1])
    )
    cross_halves = line_sum(cross_halves)
    heads_grads = [
        product(block, self_merge[0], "csd,ed->cse").astype(jnp.bfloat16) for block in merge_blocks
    ]
    query_grads, key_grads, value_grads = attend_back(
        self_queries, self_keys, self_values, own_bias, heads_grads, self_heads, self_sums
    )
    query_grads = scaled_grads(query_grads)
    self_norm_grad = own_sum(
        [
            back_rows(query_grads[step], self_weights[0])
            + back_rows(key_grads[step], self_weights[1])
            + back_rows(value_grads[step], self_weights[2])
            for step in range(model_total)
        ]
    )
    self_merge_grad = weight_sums(self_heads, merge_blocks)
    self_project_grad = jnp.stack(
        [
            weight_sums(self_blocks, query_grads),
            weight_sums(self_blocks, key_grads),
            weight_sums(self_blocks, value_grads),
        ]
    )
    self_halves = (
        pair_half(self_project_grad.astype(jnp.bfloat16)),
        pair_half(self_merge_grad.astype(jnp.bfloat16)),
    )
    rows_grad_self, gain_self_grad = layer_norm_back(
        self_norm_grad, unit_self, inverse_self, norm_self[0]
    )
    mixed_grad = first_grad + rows_grad_self
    summary_pairs, mixed_grad = lax.optimization_barrier((summary_pairs, mixed_grad))
    summary_grads = [product(left, right, "csd,cse->de") for left, right in summary_pairs]
    summary_project_grad = jnp.stack(summary_grads[:3])
    summary_merge_grad, summary_up_grad, summary_down_grad = summary_grads[3:]
    gains = jnp.stack([gain_self_grad, gain_cross_grad, gain_hidden_grad])
    firsts = jnp.concatenate(
        [normed_first.astype(jnp.float32), raw_first.astype(jnp.float32), before_first], 1
    ).reshape(-1, D)
    shared = trade(jnp.concatenate([gains, firsts]), ("dp", "mp"), False, 3)
    gains = jnp.sum(shared[:, :3], 0)
    clip_firsts = shared.reshape((-1, model_total) + shared.shape[1:])
    clip_firsts = lax.dynamic_index_in_dim(clip_firsts, model_index, 1, False)[:, 3:]
    clip_firsts = clip_firsts.reshape(clip_total, -1)
    normed_firsts = clip_firsts[:, :D].astype(jnp.bfloat16)
    raw_firsts = clip_firsts[:, D : 2 * D].astype(jnp.bfloat16)
    before_firsts = clip_firsts[:, 2 * D :]
    true_firsts = with_class(raw_firsts, view_pick)
    hidden_firsts = gelu_exact(before_firsts).astype(jnp.bfloat16)
    down_sum = pair_whole(down_half, down_grad.shape) + replaced(
        hidden_firsts, true_firsts, raw_firsts
    )
    up_sum = pair_whole(up_half, up_grad.shape) + replaced(
        normed_firsts,
        act_back(before_firsts, true_firsts, hidden_down[0]),
        act_back(before_firsts, raw_firsts, hidden_down[0]),
    )

    sent_rows = ((1.0 - mixing) * mixed_grad).astype(jnp.bfloat16)
    self_halves, cross_halves, sent_rows = lax.optimization_barrier(
        (self_halves, cross_halves, sent_rows)
    )
    self_halves = line_sum(self_halves)
    cross_project_sum = pair_whole(cross_halves[0], cross_project_grad.shape)
    cross_merge_sum = pair_whole(cross_halves[1], cross_merge_grad.shape)
    self_project_sum = pair_whole(self_halves[0], self_project_grad.shape)
    self_merge_sum = pair_whole(self_halves[1], self_merge_grad.shape)
    clips = jnp.arange(clip_total, dtype=jnp.int32)
    inverse_partner = jnp.sum(
        jnp.where(partner[None, :] == clips[:, None], clips[None, :], 0), 1
    )
    returned_rows = clip_rows(sent_rows, inverse_partner, 4).astype(jnp.float32)
    tokens_grad = (mixing * mixed_grad + returned_rows)[:, None]
    tokens_out = third_rows.astype(jnp.bfloat16)[:, None]
    return (
        tokens_out,
        summary_out,
        tokens_grad,
        self_project_sum[None],
        self_merge_sum[None],
        cross_project_sum[None],
        cross_merge_sum[None],
        up_sum[None],
        down_sum[None],
        gains[0][None],
        gains[1][None],
        gains[2][None],
        summary_project_grad,
        summary_merge_grad,
        summary_up_grad,
        summary_down_grad,
        summary_norm_self_grad,
        summary_norm_hidden_grad,
    )


def solution(mesh):
    in_specs = (
        P("dp", "view", "mp", None),
        P(),
        P("dp"),
        P(),
        P(),
        P("view", None, None, "mp"),
        P("view", "mp", None),
        P("view", None, None, "mp"),
        P("view", "mp", None),
        P("view", None, "mp"),
        P("view", "mp", None),
        P("view", None),
        P("view", None),
        P("view", None),
        P(None, None, "mp"),
        P("mp", None),
        P(None, "mp"),
        P("mp", None),
        P(),
        P(),
        P("dp", "view", "mp", None),
        P(),
    )
    out_specs = (
        P("dp", "view", "mp", None),
        P(),
        P("dp", "view", "mp", None),
        P("view", None, None, "mp"),
        P("view", "mp", None),
        P("view", None, None, "mp"),
        P("view", "mp", None),
        P("view", None, "mp"),
        P("view", "mp", None),
        P("view", None),
        P("view", None),
        P("view", None),
        P(None, None, "mp"),
        P("mp", None),
        P(None, "mp"),
        P("mp", None),
        P(),
        P(),
    )
    return jax.shard_map(shards, mesh=mesh, in_specs=in_specs, out_specs=out_specs, check_vma=False)
```

```python
import functools

import jax
import jax.numpy as jnp
from jax import lax
from jax.experimental import pallas as pl
from jax.experimental.pallas import tpu as pltpu
from jax.sharding import PartitionSpec as P

D = 768
HEAD = 64
MESH = pl.DeviceIdType.MESH


EPS = 1e-05
NEG = -1000000000.0


def shifted(value, axis, steps):
    count = lax.axis_size(axis)
    pairs = [(source, (source + steps) % count) for source in range(count)]
    return lax.ppermute(value, axis, pairs)


def layer_norm(rows, gain):
    center = rows - jnp.mean(rows, -1, keepdims=True)
    inverse = lax.rsqrt(jnp.mean(center * center, -1, keepdims=True) + EPS)
    unit = center * inverse
    return (unit * gain, unit, inverse)


def layer_norm_back(grad_out, unit, inverse, gain):
    gain_grad = jnp.sum(grad_out * unit, axis=tuple(range(grad_out.ndim - 1)))
    scaled = grad_out * gain
    centered = scaled - jnp.mean(scaled, -1, keepdims=True)
    return (inverse * (centered - unit * jnp.mean(scaled * unit, -1, keepdims=True)), gain_grad)


def gelu_exact(values):
    return jax.nn.gelu(values, approximate=False)


def product(left, right, form):
    return jnp.einsum(form, left, right, preferred_element_type=jnp.float32)


def split_heads(rows):
    return rows.reshape(rows.shape[:-1] + (rows.shape[-1] // HEAD, HEAD))


def merge_heads(rows):
    return rows.reshape(rows.shape[:-2] + (rows.shape[-2] * rows.shape[-1],))


def peer_of(axes, index):
    place = {}
    for axis in reversed(axes):
        count = lax.axis_size(axis)
        place[axis] = index % count
        index = index // count
    return place


def flat_index(axes):
    index = 0
    for axis in axes:
        index = index * lax.axis_size(axis) + lax.axis_index(axis)
    return index


def trade_kernel(axes, total, split, source, target, send_sem, recv_sem, own_sem):
    me = flat_index(axes)
    barrier = pltpu.get_barrier_semaphore()
    for step in range(1, total):
        peer = peer_of(axes, (me + step) % total)
        pl.semaphore_signal(barrier, inc=1, device_id=peer, device_id_type=MESH)
    pl.semaphore_wait(barrier, total - 1)

    def piece(index):
        return source.at[index] if split else source

    own = pltpu.make_async_copy(piece(me), target.at[me], own_sem)
    own.start()
    copies = []
    for step in range(1, total):
        to = (me + step) % total
        copies.append(
            pltpu.make_async_remote_copy(
                src_ref=piece(to),
                dst_ref=target.at[me],
                send_sem=send_sem.at[step],
                recv_sem=recv_sem.at[step],
                device_id=peer_of(axes, to),
                device_id_type=MESH,
            )
        )
        copies[-1].start()
    own.wait()
    for copy in copies:
        copy.wait()


def trade(value, axes, split, collective_id):
    total = 1
    for axis in axes:
        total *= lax.axis_size(axis)
    piece = value.shape[1:] if split else value.shape
    return pl.pallas_call(
        functools.partial(trade_kernel, axes, total, split),
        out_shape=jax.ShapeDtypeStruct((total,) + piece, value.dtype),
        in_specs=[pl.BlockSpec(memory_space=pltpu.VMEM)],
        out_specs=pl.BlockSpec(memory_space=pltpu.VMEM),
        scratch_shapes=[
            pltpu.SemaphoreType.DMA((total,)),
            pltpu.SemaphoreType.DMA((total,)),
            pltpu.SemaphoreType.DMA,
        ],
        compiler_params=pltpu.CompilerParams(collective_id=collective_id, has_side_effects=True),
    )(value)


def pick_kernel(wanted_ref, held_ref, out_ref):
    for place in range(out_ref.shape[0]):
        out_ref[place] = held_ref[wanted_ref[place]]


def pick(held, wanted):
    return pl.pallas_call(
        pick_kernel,
        in_specs=[
            pl.BlockSpec(memory_space=pltpu.SMEM),
            pl.BlockSpec(memory_space=pltpu.VMEM),
        ],
        out_specs=pl.BlockSpec(memory_space=pltpu.VMEM),
        out_shape=jax.ShapeDtypeStruct(held.shape, held.dtype),
    )(wanted, held)


def clip_total_sum(value, collective_id):
    count = lax.axis_size("dp")
    pieces = trade(value.reshape(count, -1, value.shape[-1]), ("dp",), True, collective_id)
    total = jnp.sum(pieces.astype(jnp.float32), 0).astype(jnp.bfloat16)
    return trade(total, ("dp",), False, collective_id + 1).reshape(value.shape)


def clip_rows(rows, wanted, collective_id):
    count = lax.axis_size("dp")
    clips, length, width = rows.shape
    pieces = jnp.swapaxes(rows.reshape(clips, count, length // count, width), 0, 1)
    held = trade(pieces, ("dp",), True, collective_id)
    held = held.reshape(count * clips, length // count, width)
    picked = pick(held, wanted)
    back = trade(picked.reshape(pieces.shape), ("dp",), True, collective_id + 1)
    return jnp.swapaxes(back, 0, 1).reshape(rows.shape)


def row_blocks(piece):
    count = lax.axis_size("mp")
    return [piece] + [shifted(piece, "mp", -step) for step in range(1, count)]


def own_sum(parts):
    total = parts[0]
    for step in range(1, len(parts)):
        total = total + shifted(parts[step].astype(jnp.bfloat16), "mp", step).astype(jnp.float32)
    return total


def whole_sum(value):
    parts = jnp.stack(row_blocks(value))
    if parts.shape[0] > 2:
        parts = jnp.roll(parts, lax.axis_index("mp"), 0)
    return jnp.sum(parts, 0)


def far_first(count):
    return list(range(1, count)) + [0]


def attend_block(query_block, key_rows, value_rows, valid):
    scores = jnp.where(valid, product(query_block, key_rows, "cqhe,ckhe->chqk"), NEG)
    highest = jnp.max(scores, -1, keepdims=True)
    raised = jnp.exp(scores - highest)
    totals = jnp.sum(raised, -1, keepdims=True)
    weights = (raised / totals).astype(jnp.bfloat16)
    result = product(weights, value_rows, "chqk,ckhe->cqhe").astype(jnp.bfloat16)
    return (result, highest + jnp.log(totals))


def attend_block_back(query_block, key_rows, value_rows, valid, grad_block, log_sums):
    scores = jnp.where(valid, product(query_block, key_rows, "cqhe,ckhe->chqk"), NEG)
    weights = jnp.exp(scores - log_sums)
    grad_weights = product(grad_block, value_rows, "cqhe,ckhe->chqk")
    grad_scores = (
        weights * (grad_weights - jnp.sum(weights * grad_weights, -1, keepdims=True))
    ).astype(jnp.bfloat16)
    query_grad = product(grad_scores, key_rows, "chqk,ckhe->cqhe").astype(jnp.bfloat16)
    key_grad = product(grad_scores, query_block, "chqk,cqhe->ckhe")
    value_grad = product(weights.astype(jnp.bfloat16), grad_block, "chqk,cqhe->ckhe")
    return (query_grad, key_grad, value_grad)


def joined(left, right, left_dim, right_dim):
    return lax.dot_general(
        left, right, (((left_dim,), (right_dim,)), ((), ())), preferred_element_type=jnp.float32
    )


def wide_bias(bias_ref, start, length, width):
    part = bias_ref[start : start + length, :]
    return jnp.concatenate([part] * (width // part.shape[1]), 1)


def attend_kernel(parts, chunk, query_ref, *refs):
    key_refs, value_refs = refs[:parts], refs[parts : 2 * parts]
    bias_ref, out_ref, sums_ref = refs[2 * parts :]
    length = key_refs[0].shape[1]
    for half in range(2):
        lanes = slice(HEAD * half, HEAD * half + HEAD)
        keys = [ref[0, :, lanes] for ref in key_refs]
        values = [ref[0, :, lanes] for ref in value_refs]
        for start in range(0, query_ref.shape[1], chunk):
            query = query_ref[0, start : start + chunk, lanes]
            scores = [
                joined(key, query, 1, 1) + wide_bias(bias_ref, j * length, length, chunk)
                for j, key in enumerate(keys)
            ]
            highest = functools.reduce(
                jnp.maximum, [jnp.max(score, 0, keepdims=True) for score in scores]
            )
            raised = [jnp.exp(score - highest) for score in scores]
            totals = sum(jnp.sum(part, 0, keepdims=True) for part in raised)
            result = sum(
                joined(value, part.astype(jnp.bfloat16), 0, 0)
                for value, part in zip(values, raised)
            )
            out_ref[0, start : start + chunk, lanes] = (result / totals).T.astype(jnp.bfloat16)
            sums_ref[0, 0, half : half + 1, start : start + chunk] = highest + jnp.log(totals)


def attend_back_kernel(parts, chunk, first, query_ref, grad_ref, heads_ref, sums_ref, *refs):
    key_refs, value_refs = refs[:parts], refs[parts : 2 * parts]
    bias_ref = refs[2 * parts]
    refs = refs[2 * parts + 1 :]
    held, outs = ((), refs) if first else (refs[: 2 * parts], refs[2 * parts :])
    query_grad_ref, grad_refs = outs[0], outs[1:]
    length = key_refs[0].shape[1]
    for half in range(2):
        lanes = slice(HEAD * half, HEAD * half + HEAD)
        keys = [ref[0, :, lanes] for ref in key_refs]
        values = [ref[0, :, lanes] for ref in value_refs]
        totals = [0.0 if first else ref[0, :, lanes] for ref in held] or [0.0] * (2 * parts)
        for start in range(0, query_ref.shape[1], chunk):
            rows = slice(start, start + chunk)
            query = query_ref[0, rows, lanes]
            grad = grad_ref[0, rows, lanes]
            shared = grad.astype(jnp.float32) * heads_ref[0, rows, lanes].astype(jnp.float32)
            delta = jnp.sum(shared.T, 0, keepdims=True)
            log_sums = sums_ref[0, 0, half : half + 1, rows]
            query_grad = 0.0
            for j in range(parts):
                scores = joined(keys[j], query, 1, 1) + wide_bias(
                    bias_ref, j * length, length, chunk
                )
                weights = jnp.exp(scores - log_sums)
                grad_scores = (weights * (joined(values[j], grad, 1, 1) - delta)).astype(
                    jnp.bfloat16
                )
                totals[j] = totals[j] + joined(grad_scores, query, 1, 0)
                totals[parts + j] = totals[parts + j] + joined(
                    weights.astype(jnp.bfloat16), grad, 1, 0
                )
                query_grad = query_grad + joined(keys[j], grad_scores, 0, 0)
            query_grad_ref[0, rows, lanes] = query_grad.T.astype(jnp.bfloat16)
        for total, ref in zip(totals, grad_refs):
            ref[0, :, lanes] = total.astype(ref.dtype)


def pair_spec(length):
    return pl.BlockSpec((1, length, 2 * HEAD), lambda clip, pair: (clip, 0, pair))


def sums_spec(length):
    return pl.BlockSpec((1, 1, 2, length), lambda clip, pair: (clip, pair, 0, 0))


def bias_spec(length):
    return pl.BlockSpec((length, 2 * HEAD), lambda clip, pair: (0, 0))


CHUNK = 512


def piece_count(step, length):
    return 2 if step > 0 and length % CHUNK == 0 else 1


def attend(queries, keys, values, bias):
    parts = len(keys)
    clips, length, width = queries[0].shape
    pairs = width // (2 * HEAD)
    heads = [None] * parts
    sums = [None] * parts
    for j in far_first(parts):
        count = piece_count(j, length)
        rows = length // count
        pieces = [
            pl.pallas_call(
                functools.partial(attend_kernel, parts, min(CHUNK, rows)),
                grid=(clips, pairs),
                out_shape=(
                    jax.ShapeDtypeStruct((clips, rows, width), jnp.bfloat16),
                    jax.ShapeDtypeStruct((clips, pairs, 2, rows), jnp.float32),
                ),
                in_specs=[
                    pl.BlockSpec(
                        (1, rows, 2 * HEAD), lambda clip, pair, place=place: (clip, place, pair)
                    )
                ]
                + [pair_spec(length)] * (2 * parts)
                + [bias_spec(parts * length)],
                out_specs=(pair_spec(rows), sums_spec(rows)),
            )(queries[j], *keys, *values, bias)
            for place in range(count)
        ]
        heads[j] = [piece[0] for piece in pieces]
        sums[j] = jnp.concatenate([piece[1] for piece in pieces], -1)
    return (heads, sums)


def merge_sum(heads, weight):
    total = product(heads[0][0], weight, "cse,ed->csd")
    for step in range(1, len(heads)):
        pieces = [
            shifted(product(piece, weight, "cse,ed->csd").astype(jnp.bfloat16), "mp", step)
            for piece in heads[step]
        ]
        total = total + jnp.concatenate(pieces, 1).astype(jnp.float32)
    return total


def whole_heads(heads):
    return [jnp.concatenate(pieces, 1) for pieces in heads]


def attend_back(queries, keys, values, bias, grads, heads, sums):
    parts = len(keys)
    clips, length, width = queries[0].shape
    pairs = width // (2 * HEAD)
    query_grads = []
    held = []
    for j in range(parts):
        kind = jnp.bfloat16 if j == parts - 1 else jnp.float32
        outs = pl.pallas_call(
            functools.partial(attend_back_kernel, parts, min(CHUNK, length), j == 0),
            grid=(clips, pairs),
            out_shape=[jax.ShapeDtypeStruct((clips, length, width), jnp.bfloat16)]
            + [jax.ShapeDtypeStruct((clips, length, width), kind)] * (2 * parts),
            in_specs=[pair_spec(length)] * 3
            + [sums_spec(length)]
            + [pair_spec(length)] * (2 * parts)
            + [bias_spec(parts * length)]
            + [pair_spec(length)] * len(held),
            out_specs=[pair_spec(length)] * (1 + 2 * parts),
        )(queries[j], grads[j], heads[j], sums[j], *keys, *values, bias, *held)
        query_grads.append(outs[0])
        held = list(outs[1:])
    return (query_grads, held[:parts], held[parts:])


def act_back(before, rows, weight):
    grad = product(rows, weight, "...d,fd->...f")
    return jax.vjp(gelu_exact, before)[1](grad)[0].astype(jnp.bfloat16)


def first_row(blocks, owners):
    row = blocks[0][:, 0]
    for block, owner in zip(blocks[1:], owners[1:]):
        row = jnp.where(owner == 0, block[:, 0], row)
    return row


def with_class(rows, class_rows):
    return (rows.astype(jnp.float32) + class_rows).astype(jnp.bfloat16)


def replaced(left, fresh, stale):
    return product(
        jnp.concatenate([left, -left]), jnp.concatenate([fresh, stale]), "ca,cb->ab"
    )


def project_rows(source, weight):
    return product(source, weight, "csd,de->cse")


def query_rows(source, weight):
    return (project_rows(source, weight) * HEAD ** (-0.5)).astype(jnp.bfloat16)


def back_rows(grad, weight):
    return product(grad, weight, "cse,de->csd")


def weight_sums(sources, grads):
    return sum(product(source, grad, "csd,cse->de") for source, grad in zip(sources, grads))


def scaled_grads(grads):
    return [grad * HEAD ** (-0.5) for grad in grads]


def summary_layer(
    summary_rows, top_grad, weights, gain_top, gain_last, summary_valid
):
    use_project, use_merge, use_up, use_down = weights
    top_normed, top_unit, top_inverse = layer_norm(summary_rows, gain_top)
    top_low = top_normed.astype(jnp.bfloat16)[None]
    top_query = query_rows(top_low, use_project[0])
    top_key = project_rows(top_low, use_project[1]).astype(jnp.bfloat16)
    top_value = project_rows(top_low, use_project[2]).astype(jnp.bfloat16)
    top_key, top_value = split_heads(top_key), split_heads(top_value)
    top_heads, top_sums = attend_block(split_heads(top_query), top_key, top_value, summary_valid)
    top_flat = merge_heads(top_heads)
    summary_mid = summary_rows + whole_sum(product(top_flat, use_merge, "cse,ed->csd")[0])
    mid_normed, mid_unit, mid_inverse = layer_norm(summary_mid, gain_last)
    mid_low = mid_normed.astype(jnp.bfloat16)[None]
    top_before = product(mid_low, use_up, "csd,df->csf")
    top_hidden = gelu_exact(top_before).astype(jnp.bfloat16)
    summary_final = summary_mid + whole_sum(product(top_hidden, use_down, "csf,fd->csd")[0])
    down_input = top_grad.astype(jnp.bfloat16)[None]
    act_grad = jax.vjp(gelu_exact, top_before)[1](product(down_input, use_down, "csd,fd->csf"))[
        0
    ].astype(jnp.bfloat16)
    mid_rows_grad, last_gain_grad = layer_norm_back(
        whole_sum(product(act_grad, use_up, "csf,df->csd")[0]), mid_unit, mid_inverse, gain_last
    )
    mid_grad = top_grad + mid_rows_grad
    merge_input = mid_grad.astype(jnp.bfloat16)[None]
    top_heads_grad = product(merge_input, use_merge, "csd,ed->cse").astype(jnp.bfloat16)
    query_grad, key_grad, value_grad = attend_block_back(
        split_heads(top_query),
        top_key,
        top_value,
        summary_valid,
        split_heads(top_heads_grad),
        top_sums,
    )
    query_grad = merge_heads(query_grad)
    key_grad = merge_heads(key_grad).astype(jnp.bfloat16)
    value_grad = merge_heads(value_grad).astype(jnp.bfloat16)
    query_grad = query_grad * HEAD ** (-0.5)
    project_terms = (
        back_rows(query_grad, use_project[0])
        + back_rows(key_grad, use_project[1])
        + back_rows(value_grad, use_project[2])
    )
    first_top_grad, top_gain_grad = layer_norm_back(
        whole_sum(project_terms[0]), top_unit, top_inverse, gain_top
    )
    class_grad = mid_grad + first_top_grad
    return (
        summary_final,
        class_grad,
        (
            (top_low, query_grad),
            (top_low, key_grad),
            (top_low, value_grad),
            (top_flat, merge_input),
            (mid_low, act_grad),
            (top_hidden, down_input),
        ),
        top_gain_grad,
        last_gain_grad,
    )


def shards(
    tokens,
    partner,
    mix_weight,
    video_ids,
    view_counts,
    self_project,
    self_merge,
    cross_project,
    cross_merge,
    hidden_up,
    hidden_down,
    norm_self,
    norm_cross,
    norm_hidden,
    summary_project,
    summary_merge,
    summary_up,
    summary_down,
    summary_norm_self,
    summary_norm_hidden,
    tokens_cotangent,
    summary_cotangent,
):
    local_tokens = tokens[:, 0]
    clip_count = local_tokens.shape[0]
    data_index = lax.axis_index("dp")
    view_index = lax.axis_index("view")
    model_index = lax.axis_index("mp")
    view_total = lax.axis_size("view")
    model_total = lax.axis_size("mp")
    clip_total = clip_count * lax.axis_size("dp")
    length = local_tokens.shape[1]
    order = far_first(model_total)
    own_clips = data_index * clip_count + jnp.arange(clip_count, dtype=jnp.int32)
    partner_tokens = clip_rows(local_tokens, partner, 0).astype(jnp.float32)
    grad_blocks = row_blocks(tokens_cotangent[:, 0])
    mixing = mix_weight[:, None, None]
    mixed_rows = mixing * local_tokens.astype(jnp.float32) + (1.0 - mixing) * partner_tokens
    owners = [(model_index + step) % model_total for step in range(model_total)]
    positions = jnp.concatenate([owner * length + jnp.arange(length) for owner in owners])
    own_valid = positions < view_counts[view_index]
    next_valid = positions < view_counts[(view_index + 1) % view_total]
    own_bias, next_bias = (
        jnp.broadcast_to(jnp.where(valid, 0.0, NEG)[:, None], (positions.shape[0], 2 * HEAD))
        for valid in (own_valid, next_valid)
    )

    normed_self, unit_self, inverse_self = layer_norm(mixed_rows, norm_self[0])
    self_blocks = row_blocks(normed_self.astype(jnp.bfloat16))
    self_weights = self_project[0]
    self_queries = [query_rows(block, self_weights[0]) for block in self_blocks]
    self_keys = [project_rows(block, self_weights[1]).astype(jnp.bfloat16) for block in self_blocks]
    self_values = [
        project_rows(block, self_weights[2]).astype(jnp.bfloat16) for block in self_blocks
    ]
    self_heads, self_sums = attend(self_queries, self_keys, self_values, own_bias)
    first_rows = mixed_rows + merge_sum(self_heads, self_merge[0])
    self_heads = whole_heads(self_heads)

    normed_cross, unit_cross, inverse_cross = layer_norm(first_rows, norm_cross[0])
    cross_blocks = row_blocks(normed_cross.astype(jnp.bfloat16))
    next_blocks = [shifted(block, "view", -1) for block in cross_blocks]
    cross_weights = cross_project[0]
    cross_queries = [query_rows(block, cross_weights[0]) for block in cross_blocks]
    cross_keys = [
        project_rows(block, cross_weights[1]).astype(jnp.bfloat16) for block in next_blocks
    ]
    cross_values = [
        project_rows(block, cross_weights[2]).astype(jnp.bfloat16) for block in next_blocks
    ]
    cross_heads, cross_sums = attend(cross_queries, cross_keys, cross_values, next_bias)
    second_rows = first_rows + merge_sum(cross_heads, cross_merge[0])
    cross_heads = whole_heads(cross_heads)

    normed_hidden, unit_hidden, inverse_hidden = layer_norm(second_rows, norm_hidden[0])
    hidden_blocks = row_blocks(normed_hidden.astype(jnp.bfloat16))
    normed_first = first_row(hidden_blocks, owners)
    before_first = product(normed_first, hidden_up[0], "cd,df->cf")
    raw_first = first_row(grad_blocks, owners)
    class_term = whole_sum(
        product(gelu_exact(before_first).astype(jnp.bfloat16), hidden_down[0], "cf,fd->cd")
    )
    befores = [product(block, hidden_up[0], "csd,df->csf") for block in hidden_blocks]
    hiddens = [gelu_exact(before).astype(jnp.bfloat16) for before in befores]
    third_rows = second_rows + own_sum(
        [product(hidden, hidden_down[0], "csf,fd->csd") for hidden in hiddens]
    )

    down_rows = grad_blocks
    act_grads = [act_back(before, rows, hidden_down[0]) for before, rows in zip(befores, down_rows)]
    hidden_norm_grad = own_sum(
        [product(act_grad, hidden_up[0], "csf,df->csd") for act_grad in act_grads]
    )
    down_grad = sum(product(h, r, "csf,csd->fd") for h, r in zip(hiddens, down_rows))
    up_grad = sum(product(b, g, "csd,csf->df") for b, g in zip(hidden_blocks, act_grads))
    up_sum, down_sum = lax.psum(
        (up_grad.astype(jnp.bfloat16), down_grad.astype(jnp.bfloat16)), "dp"
    )
    everyone = ("dp", "view", "mp")
    class_all = trade(second_rows[:, 0] + class_term, everyone, False, 2)
    class_all = class_all.reshape(clip_total // clip_count, view_total, model_total, clip_count, D)
    class_grid = jnp.swapaxes(class_all[:, :, 0], 1, 2).reshape(clip_total, view_total, D)
    row_total = clip_total * view_total
    token_video = jnp.repeat(video_ids, view_total)
    summary_valid = (token_video[:, None] == token_video[None, :])[None, None]
    summary_final, class_flat, summary_pairs, summary_norm_self_grad, summary_norm_hidden_grad = (
        summary_layer(
            class_grid.reshape(row_total, D),
            summary_cotangent.reshape(row_total, D),
            (summary_project, summary_merge, summary_up, summary_down),
            summary_norm_self,
            summary_norm_hidden,
            summary_valid,
        )
    )
    summary_out = summary_final.reshape(clip_total, view_total, D)
    clip_match = (jnp.arange(clip_total, dtype=jnp.int32)[:, None] == own_clips[None, :]).astype(
        jnp.float32
    )
    view_match = (jnp.arange(view_total) == view_index).astype(jnp.float32)
    class_grad = class_flat.reshape(clip_total, view_total, D)
    view_pick = jnp.sum(class_grad * view_match[None, :, None], axis=1)
    own_class = jnp.sum(clip_match[:, :, None] * view_pick[:, None, :], axis=0)

    third_grad = tokens_cotangent[:, 0].astype(jnp.float32)
    at_first = (jnp.arange(length)[None, :, None] == 0) & (model_index == 0)
    third_grad = third_grad + jnp.where(at_first, own_class[:, None], 0.0)
    true_act = act_back(before_first, with_class(raw_first, own_class), hidden_down[0])
    true_term = whole_sum(product(true_act, hidden_up[0], "cf,df->cd"))
    hidden_norm_grad = jnp.where(at_first, true_term[:, None], hidden_norm_grad)
    rows_grad_hidden, gain_hidden_grad = layer_norm_back(
        hidden_norm_grad, unit_hidden, inverse_hidden, norm_hidden[0]
    )
    second_grad = third_grad + rows_grad_hidden

    merge_blocks = row_blocks(second_grad.astype(jnp.bfloat16))
    heads_grads = [
        product(block, cross_merge[0], "csd,ed->cse").astype(jnp.bfloat16)
        for block in merge_blocks
    ]
    query_grads, key_grads, value_grads = attend_back(
        cross_queries, cross_keys, cross_values, next_bias, heads_grads, cross_heads, cross_sums
    )
    query_grads = scaled_grads(query_grads)
    terms = [None] * model_total
    for step in order:
        next_term = back_rows(key_grads[step], cross_weights[1]) + back_rows(
            value_grads[step], cross_weights[2]
        )
        returned = shifted(next_term.astype(jnp.bfloat16), "view", 1).astype(jnp.float32)
        terms[step] = back_rows(query_grads[step], cross_weights[0]) + returned
    cross_norm_grad = own_sum(terms)
    cross_merge_grad = weight_sums(cross_heads, merge_blocks)
    cross_project_grad = jnp.stack(
        [
            weight_sums(cross_blocks, query_grads),
            weight_sums(next_blocks, key_grads),
            weight_sums(next_blocks, value_grads),
        ]
    )
    cross_low = cross_project_grad.astype(jnp.bfloat16)
    rows_grad_cross, gain_cross_grad = layer_norm_back(
        cross_norm_grad, unit_cross, inverse_cross, norm_cross[0]
    )
    first_grad = second_grad + rows_grad_cross

    merge_blocks = row_blocks(first_grad.astype(jnp.bfloat16))
    heads_grads = [
        product(block, self_merge[0], "csd,ed->cse").astype(jnp.bfloat16) for block in merge_blocks
    ]
    query_grads, key_grads, value_grads = attend_back(
        self_queries, self_keys, self_values, own_bias, heads_grads, self_heads, self_sums
    )
    query_grads = scaled_grads(query_grads)
    self_norm_grad = own_sum(
        [
            back_rows(query_grads[step], self_weights[0])
            + back_rows(key_grads[step], self_weights[1])
            + back_rows(value_grads[step], self_weights[2])
            for step in range(model_total)
        ]
    )
    self_merge_grad = weight_sums(self_heads, merge_blocks)
    self_project_grad = jnp.stack(
        [
            weight_sums(self_blocks, query_grads),
            weight_sums(self_blocks, key_grads),
            weight_sums(self_blocks, value_grads),
        ]
    )
    self_low = self_project_grad.astype(jnp.bfloat16)
    rows_grad_self, gain_self_grad = layer_norm_back(
        self_norm_grad, unit_self, inverse_self, norm_self[0]
    )
    mixed_grad = first_grad + rows_grad_self
    summary_pairs, mixed_grad = lax.optimization_barrier((summary_pairs, mixed_grad))
    summary_grads = [product(left, right, "csd,cse->de") for left, right in summary_pairs]
    summary_project_grad = jnp.stack(summary_grads[:3])
    summary_merge_grad, summary_up_grad, summary_down_grad = summary_grads[3:]
    gains = jnp.stack([gain_self_grad, gain_cross_grad, gain_hidden_grad])
    sent_rows = ((1.0 - mixing) * mixed_grad).astype(jnp.bfloat16)
    self_low, up_sum, down_sum, sent_rows = lax.optimization_barrier(
        (self_low, up_sum, down_sum, sent_rows)
    )
    cross_project_sum, self_project_sum = lax.psum((cross_low, self_low), "dp")
    clips = jnp.arange(clip_total, dtype=jnp.int32)
    inverse_partner = jnp.sum(
        jnp.where(partner[None, :] == clips[:, None], clips[None, :], 0), 1
    )
    returned_rows = clip_rows(sent_rows, inverse_partner, 4).astype(jnp.float32)
    merge_low = jnp.concatenate([cross_merge_grad, self_merge_grad]).astype(jnp.bfloat16)
    merge_low, gains, returned_rows = lax.optimization_barrier((merge_low, gains, returned_rows))
    firsts = jnp.concatenate(
        [normed_first.astype(jnp.float32), raw_first.astype(jnp.float32), before_first], 1
    ).reshape(-1, D)
    shared = trade(jnp.concatenate([gains, firsts]), ("dp", "mp"), False, 3)
    gains = jnp.sum(shared[:, :3], 0)
    clip_firsts = shared.reshape((-1, model_total) + shared.shape[1:])
    clip_firsts = lax.dynamic_index_in_dim(clip_firsts, model_index, 1, False)[:, 3:]
    clip_firsts = clip_firsts.reshape(clip_total, -1)
    normed_firsts = clip_firsts[:, :D].astype(jnp.bfloat16)
    raw_firsts = clip_firsts[:, D : 2 * D].astype(jnp.bfloat16)
    before_firsts = clip_firsts[:, 2 * D :]
    true_firsts = with_class(raw_firsts, view_pick)
    hidden_firsts = gelu_exact(before_firsts).astype(jnp.bfloat16)
    down_sum = down_sum.astype(jnp.float32) + replaced(
        hidden_firsts, true_firsts, raw_firsts
    )
    up_sum = up_sum.astype(jnp.float32) + replaced(
        normed_firsts,
        act_back(before_firsts, true_firsts, hidden_down[0]),
        act_back(before_firsts, raw_firsts, hidden_down[0]),
    )

    cross_merge_sum, self_merge_sum = jnp.split(clip_total_sum(merge_low, 6), 2)
    tokens_grad = (mixing * mixed_grad + returned_rows)[:, None]
    tokens_out = third_rows.astype(jnp.bfloat16)[:, None]
    return (
        tokens_out,
        summary_out,
        tokens_grad,
        self_project_sum.astype(jnp.float32)[None],
        self_merge_sum.astype(jnp.float32)[None],
        cross_project_sum.astype(jnp.float32)[None],
        cross_merge_sum.astype(jnp.float32)[None],
        up_sum[None],
        down_sum[None],
        gains[0][None],
        gains[1][None],
        gains[2][None],
        summary_project_grad,
        summary_merge_grad,
        summary_up_grad,
        summary_down_grad,
        summary_norm_self_grad,
        summary_norm_hidden_grad,
    )


def solution(mesh):
    in_specs = (
        P("dp", "view", "mp", None),
        P(),
        P("dp"),
        P(),
        P(),
        P("view", None, None, "mp"),
        P("view", "mp", None),
        P("view", None, None, "mp"),
        P("view", "mp", None),
        P("view", None, "mp"),
        P("view", "mp", None),
        P("view", None),
        P("view", None),
        P("view", None),
        P(None, None, "mp"),
        P("mp", None),
        P(None, "mp"),
        P("mp", None),
        P(),
        P(),
        P("dp", "view", "mp", None),
        P(),
    )
    out_specs = (
        P("dp", "view", "mp", None),
        P(),
        P("dp", "view", "mp", None),
        P("view", None, None, "mp"),
        P("view", "mp", None),
        P("view", None, None, "mp"),
        P("view", "mp", None),
        P("view", None, "mp"),
        P("view", "mp", None),
        P("view", None),
        P("view", None),
        P("view", None),
        P(None, None, "mp"),
        P("mp", None),
        P(None, "mp"),
        P("mp", None),
        P(),
        P(),
    )
    return jax.shard_map(shards, mesh=mesh, in_specs=in_specs, out_specs=out_specs, check_vma=False)
```
